256 devices in a mesh: dp: 32 (over z_hi, y, core), mp: 8 (over z_lo, x).
Axes of the slice: x: 4, y: 4, z: 8 (z_hi: 4, z_lo: 2; z = z_hi * 2 + z_lo), core: 2. Of those that a mesh axis runs over, the one named last changes fastest.
Arguments:
- features: bfloat16 [4096, 4608], P('dp'), may hold values from -6 to 6
- proj_in: bfloat16 [4608, 2560], P('dp', 'mp'), may hold values from -0.09375 to 0.09375
- proj_out: bfloat16 [2560, 2560], P('mp'), may hold values from -0.125 to 0.125
- expert_gate: bfloat16 [64, 2560, 1536], P('dp', None, 'mp'), may hold values from -0.125 to 0.125
- expert_up: bfloat16 [64, 2560, 1536], P('dp', None, 'mp'), may hold values from -0.125 to 0.125
- expert_down: bfloat16 [64, 1536, 2560], P('dp', 'mp'), may hold values from -0.15625 to 0.15625
- routes: int32 [4096, 6], P('dp'), may hold values from 0 to 63, all different within a row; in each aligned block of 128 rows (0 to 127, 128 to 255, ...) at most 15 rows name the same one
- gate_weights: float32 [4096, 6], P('dp'), may hold values from 0.1 to 0.6
- cotangent: bfloat16 [4096, 2560], P('dp'), may hold values from -0.09375 to 0.09375
- first_in: float32 [4608, 2560], P('dp', 'mp'), may hold values from -2 to 2
- second_in: float32 [4608, 2560], P('dp', 'mp'), may hold values from 0.02 to 1
- first_out: float32 [2560, 2560], P('mp', 'dp'), may hold values from -2 to 2
- second_out: float32 [2560, 2560], P('mp', 'dp'), may hold values from 0.02 to 1
Outputs:
- moe_out: bfloat16 [4096, 2560], P('dp')
- new_proj_in: bfloat16 [4608, 2560], P('dp', 'mp')
- new_proj_out: bfloat16 [2560, 2560], P('mp', 'dp')
- new_first_in: float32 [4608, 2560], P('dp', 'mp')
- new_second_in: float32 [4608, 2560], P('dp', 'mp')
- new_first_out: float32 [2560, 2560], P('mp', 'dp')
- new_second_out: float32 [2560, 2560], P('mp', 'dp')
The draws below stay inside these ranges and needn't reach their ends.
Inputs may be any that keep to these rules, and one draw needn't show every extreme that they name: `routes`: each row names 6 different experts. Within the rows of one device (aligned blocks of 128 rows) no expert is named more than 15 times, and in every draw some expert is named exactly 15 times in some block.
All inputs are finite; a program needn't handle non-finite values.
Results may differ from the reference program's by a relative error of at most 0.01.
Values may be sent and summed in bfloat16 or wider, within the bound.
No kernel may reach another device: no remote copies, remote signals or barrier semaphores. Data moves between devices by JAX's collectives and lax.ppermute only.
A program may use at most 128 MiB of HBM per device.

```python
import math
import jax
import jax.numpy as jnp
import numpy as np
from jax import lax

VIS = 4608
HID = 2560
D = 2560
EXPERTS = 64
FE = 1536
TOP = 6
TOK_DEV = 128
CAP = 15
TOKENS = 4096
N_DP = 32
N_MP = 8


def steps_of(key, dims, shards, least, largest):
    factor_of = 1.0
    for dim, blocks in shards:
        steps = jax.random.uniform(jax.random.fold_in(jax.random.fold_in(key, 6), dim), (blocks,), jnp.float32, least / len(shards), largest / len(shards))
        factor_of = factor_of * jnp.repeat(jnp.exp(steps), dims[dim] // blocks).reshape((-1,) + (1,) * (len(dims) - 1 - dim))
    return factor_of


def assign_block(rng, own, number, rows, count, top, bound, skew):
    order = jax.random.permutation(rng, count)
    crowded, usual = shares(count, rows * top, bound, skew, True), shares(count, rows * top, bound, skew, False)
    places = jnp.arange(count)

    def named(lengths, rotation):
        used = int((lengths > 0).sum())
        fixed = max(1, used // 4)
        shifted = fixed + (places - fixed + rotation * (used - fixed)) % max(1, count - fixed)
        return jnp.zeros((count,), jnp.int32).at[order[jnp.where(places < fixed, places, shifted)]].set(jnp.asarray(lengths, jnp.int32))

    lengths = jnp.where(number % 4 == 0, named(crowded, number // 4), named(usual, number - number // 4 - 1))
    mixed = jax.random.permutation(jax.random.fold_in(own, 3), count)
    source_of, taker = mixed[0:count // 2 * 2:2], mixed[1:count // 2 * 2:2]
    slack = jnp.minimum(lengths[source_of] - 1, bound - lengths[taker]) // 2
    slack = jnp.where((source_of == order[0]) | (taker == order[0]) | (lengths[taker] == 0), 0, jnp.maximum(slack, 0))
    shifted = jax.random.randint(jax.random.fold_in(own, 4), (count // 2,), 0, 1 << 20) % (slack + 1)
    lengths = lengths.at[source_of].add(-shifted).at[taker].add(shifted)
    labels = jnp.searchsorted(jnp.cumsum(lengths), jnp.arange(rows * top), side="right").astype(jnp.int32)
    table = labels.reshape(top, rows).T
    table = table[jax.random.permutation(jax.random.fold_in(own, 1), rows)]
    rotation = jax.random.randint(jax.random.fold_in(own, 2), (rows, 1), 0, top)
    return jnp.take_along_axis(table, (jnp.arange(top)[None, :] + rotation) % top, axis=1)


def shares(number_of, total, limit, lean, full):
    loads = [(1 << 20) // math.isqrt(standing ** lean) + 1 for standing in range(1, number_of + 1)]
    largest = limit if full else min(limit, max(-(-total // number_of), total * loads[0] // sum(loads)))
    least = 1 if total - largest >= number_of - 1 else 0
    counts, surplus = [largest] + [least] * (number_of - 1), total - largest - least * (number_of - 1)
    while surplus > 0:
        candidates = [i for i in range(1, number_of) if counts[i] < largest] or [i for i in range(1, number_of) if counts[i] < limit]
        mass, remaining = sum([loads[i] for i in candidates]), surplus
        for i in candidates:
            extra = min(limit - counts[i], max(1, remaining * loads[i] // mass), surplus)
            counts[i] = counts[i] + extra
            surplus = surplus - extra
    return np.array(counts)


def scatter_about(stream_key, shape, deviation, most, shards=(), held_as=jnp.bfloat16):
    values = jax.random.normal(stream_key, shape, jnp.float32) * deviation
    if len(shards) > 0:
        values = steps_of(stream_key, shape, shards, -0.22, 0.18) * values
    return jnp.clip(values, min=-most, max=most).astype(held_as)


def setup_inputs(seed: int = 0) -> dict:
    keys = jax.random.split(jax.random.key(seed), 14)
    features = scatter_about(keys[0], (TOKENS, VIS), 1.0, 6.0, ((0, 32),))
    proj_in = scatter_about(keys[1], (VIS, HID), VIS ** -0.5, 0.09375, ((0, 32), (1, 8)))
    proj_out = scatter_about(keys[2], (HID, D), HID ** -0.5, 0.125, ((0, 8),))
    expert_gate = scatter_about(keys[3], (EXPERTS, D, FE), D ** -0.5, 0.125, ((0, 32), (2, 8)))
    expert_up = scatter_about(keys[4], (EXPERTS, D, FE), D ** -0.5, 0.125, ((0, 32), (2, 8)))
    expert_down = scatter_about(keys[5], (EXPERTS, FE, D), FE ** -0.5, 0.15625, ((0, 32), (1, 8)))
    routes_keys = jax.random.split(jax.random.fold_in(keys[6], 1), TOKENS // TOK_DEV)
    routes_turns = jax.random.permutation(jax.random.fold_in(keys[6], 3), TOKENS // TOK_DEV)
    routes = jax.vmap(lambda own, number: assign_block(jax.random.fold_in(keys[6], 2), own, number, TOK_DEV, EXPERTS, TOP, CAP, 2))(routes_keys, routes_turns).reshape((TOKENS, TOP))
    gate_weights = jnp.clip(0.1 + 0.5 * jax.random.uniform(keys[7], (TOKENS, TOP), jnp.float32) ** steps_of(keys[7], (TOKENS, TOP), ((0, 32),), -0.2, 0.2), 0.1, 0.6)
    cotangent = scatter_about(keys[8], (TOKENS, D), 0.015625, 0.09375, ((0, 32),))
    first_in = scatter_about(keys[9], (VIS, HID), 0.3, 2.0, ((0, 32), (1, 8)), jnp.float32)
    second_in = jnp.clip(jnp.exp(math.log(1.0) - 3.912023 * jax.random.uniform(keys[10], (VIS, HID), jnp.float32) ** steps_of(keys[10], (VIS, HID), ((0, 32), (1, 8)), -0.2, 0.2)), 0.02, 1.0)
    first_out = scatter_about(keys[11], (HID, D), 0.3, 2.0, ((0, 8), (1, 32)), jnp.float32)
    second_out = jnp.clip(jnp.exp(math.log(1.0) - 3.912023 * jax.random.uniform(keys[12], (HID, D), jnp.float32) ** steps_of(keys[12], (HID, D), ((0, 8), (1, 32)), -0.2, 0.2)), 0.02, 1.0)
    return {"features": features, "proj_in": proj_in, "proj_out": proj_out, "expert_gate": expert_gate, "expert_up": expert_up, "expert_down": expert_down, "routes": routes, "gate_weights": gate_weights, "cotangent": cotangent, "first_in": first_in, "second_in": second_in, "first_out": first_out, "second_out": second_out}


BETA_ONE = 0.9
BETA_TWO = 0.999
EPSILON = 1e-08
LEARN_RATE = 0.001
WEIGHT_DECAY = 0.1
FIRST_FIX = 1.0 - 0.9 ** 50 * 0.9 ** 50
SECOND_FIX = 1.0 - 0.999 ** 50 * 0.999 ** 50

def gelu_parts(preact):

    def smooth(values):
        return jax.nn.gelu(values, approximate=True)
    result, pullback = jax.vjp(smooth, preact)
    return (result, pullback(jnp.ones_like(preact))[0])

def slot_table(chosen_block):
    chosen = chosen_block.reshape(-1)
    onehot = (chosen[:, None] == jnp.arange(EXPERTS, dtype=jnp.int32)[None, :]).astype(jnp.int32)
    earlier = jnp.cumsum(onehot, axis=0) - onehot
    return (chosen, lax.optimization_barrier(jnp.sum(earlier * onehot, axis=1)).astype(jnp.int32))

def adamw_update(weight, gradient, first, second):
    first_new = BETA_ONE * first + (1.0 - BETA_ONE) * gradient
    second_new = BETA_TWO * second + (1.0 - BETA_TWO) * gradient * gradient
    update = first_new / FIRST_FIX / (jnp.sqrt(second_new / SECOND_FIX) + EPSILON)
    current = weight.astype(jnp.float32)
    return ((current - LEARN_RATE * (update + WEIGHT_DECAY * current)).astype(jnp.bfloat16), first_new, second_new)

def expert_pass(pieces):
    inputs, grads_in, w_gate, w_up, w_down = pieces
    inner_width = w_gate.shape[1] // N_MP
    gate_weight_matrix = w_gate.astype(jnp.float32).reshape(D, N_MP, inner_width)
    up_weight_matrix = w_up.astype(jnp.float32).reshape(D, N_MP, inner_width)
    down_weight_matrix = w_down.astype(jnp.float32).reshape(N_MP, inner_width, D)
    input_wide_rows = inputs.astype(jnp.float32)
    gradient_wide_rows = grads_in.astype(jnp.float32)
    gate_projection = jnp.einsum('ny,yhs->hns', input_wide_rows, gate_weight_matrix)
    up_projection = jnp.einsum('ny,yhs->hns', input_wide_rows, up_weight_matrix)
    sigmoid_gate = jax.nn.sigmoid(gate_projection)
    silu_gate = gate_projection * sigmoid_gate
    inner_activation = (silu_gate * up_projection).astype(jnp.bfloat16)
    output_portions = jnp.einsum('pex,pxi->pei', inner_activation.astype(jnp.float32), down_weight_matrix).astype(jnp.bfloat16)
    down_weight_gradient = jnp.einsum('sb,zab->zsa', gradient_wide_rows, down_weight_matrix)
    gate_weight_gradient = (down_weight_gradient * up_projection * sigmoid_gate * (1.0 + gate_projection * (1.0 - sigmoid_gate))).astype(jnp.bfloat16)
    up_weight_gradient = (down_weight_gradient * silu_gate).astype(jnp.bfloat16)
    input_portions = (jnp.einsum('swv,osv->swo', gate_weight_gradient.astype(jnp.float32), gate_weight_matrix) + jnp.einsum('swv,osv->swo', up_weight_gradient.astype(jnp.float32), up_weight_matrix)).astype(jnp.bfloat16)
    return (lax.optimization_barrier(jnp.sum(output_portions.astype(jnp.float32), axis=0)), lax.optimization_barrier(jnp.sum(input_portions.astype(jnp.float32), axis=0)))

def reference(features, proj_in, proj_out, expert_gate, expert_up, expert_down, routes, gate_weights, cotangent, first_in, second_in, first_out, second_out):
    preact = jnp.dot(features, proj_in, preferred_element_type=jnp.float32)
    activated, gelu_slope = gelu_parts(preact)
    hidden = activated.astype(jnp.bfloat16)
    mapped = jnp.dot(hidden, proj_out, preferred_element_type=jnp.float32).astype(jnp.bfloat16)
    chosen, slot_index = jax.vmap(slot_table)(routes.reshape(N_DP, TOK_DEV, TOP))
    source = jnp.arange(N_DP, dtype=jnp.int32)[:, None]
    position = ((chosen * N_DP + source) * CAP + slot_index).reshape(-1).astype(jnp.int32)
    weights = gate_weights.reshape(-1, 1)
    spread = jnp.repeat(mapped, TOP, axis=0)
    gated_rows = (weights * jnp.repeat(cotangent.astype(jnp.float32), TOP, axis=0)).astype(jnp.bfloat16)
    total_slots = EXPERTS * N_DP * CAP
    slot_inputs = jnp.zeros((total_slots, D), jnp.bfloat16).at[position].set(spread).reshape(EXPERTS, N_DP * CAP, D)
    slot_grads = jnp.zeros((total_slots, D), jnp.bfloat16).at[position].set(gated_rows).reshape(EXPERTS, N_DP * CAP, D)
    expert_outputs, expert_inputs = lax.map(expert_pass, (slot_inputs, slot_grads, expert_gate, expert_up, expert_down))
    back_out = expert_outputs.reshape(total_slots, D)[position]
    back_in = expert_inputs.reshape(total_slots, D)[position]
    moe_out = (mapped.astype(jnp.float32) + lax.optimization_barrier(jnp.sum((weights * back_out).reshape(TOKENS, TOP, D), axis=1))).astype(jnp.bfloat16)
    grad_mapped = (cotangent.astype(jnp.float32) + lax.optimization_barrier(jnp.sum(back_in.reshape(TOKENS, TOP, D), axis=1))).astype(jnp.bfloat16)
    grad_pre = (jnp.dot(grad_mapped, proj_out.T, preferred_element_type=jnp.float32) * gelu_slope).astype(jnp.bfloat16)

    def block_sum(carry, pieces):
        feature_block, pre_block, hidden_block, mapped_block = pieces
        term_in = jnp.dot(feature_block.T, pre_block, preferred_element_type=jnp.float32).astype(jnp.bfloat16)
        term_out = jnp.dot(hidden_block.T, mapped_block, preferred_element_type=jnp.float32).astype(jnp.bfloat16)
        term_in = lax.optimization_barrier(term_in).astype(jnp.float32)
        term_out = lax.optimization_barrier(term_out).astype(jnp.float32)
        return ((carry[0] + term_in, carry[1] + term_out), jnp.zeros((), jnp.float32))
    start_sums = (jnp.zeros((VIS, HID), jnp.float32), jnp.zeros((HID, D), jnp.float32))
    grad_pair, unused = lax.scan(block_sum, start_sums, (features.reshape(N_DP, TOK_DEV, VIS), grad_pre.reshape(N_DP, TOK_DEV, HID), hidden.reshape(N_DP, TOK_DEV, HID), grad_mapped.reshape(N_DP, TOK_DEV, D)))
    new_in, first_in_new, second_in_new = adamw_update(proj_in, grad_pair[0], first_in, second_in)
    new_out, first_out_new, second_out_new = adamw_update(proj_out, grad_pair[1], first_out, second_out)
    return (moe_out, new_in, new_out, first_in_new, second_in_new, first_out_new, second_out_new)
```

```python
import jax
import jax.numpy as jnp
from jax import lax
from jax.experimental import pallas as pl
from jax.experimental.pallas import tpu as pltpu
from jax.sharding import PartitionSpec as P

EXPERTS = 64
TOP = 6
SLOTS = 16
NX, NZ = 4, 2
RY, RZ = 4, 4

BETA_ONE = 0.9
BETA_TWO = 0.999
EPSILON = 1e-08
LEARN_RATE = 0.001
WEIGHT_DECAY = 0.1
FIRST_FIX = 1.0 - 0.9**50 * 0.9**50
SECOND_FIX = 1.0 - 0.999**50 * 0.999**50

BF = jnp.bfloat16
F32 = jnp.float32


def mp_send(v, dx, dz=0):
    pairs = [
        (z * NX + x, (z + dz) % NZ * NX + (x + dx) % NX) for z in range(NZ) for x in range(NX)
    ]
    return lax.ppermute(v, "mp", pairs)


def dp_send(v, dz=0, dy=0, dc=0):
    pairs = [
        ((z * RY + y) * 2 + c, ((z + dz) % RZ * RY + (y + dy) % RY) * 2 + (c + dc) % 2)
        for z in range(RZ)
        for y in range(RY)
        for c in range(2)
    ]
    return lax.ppermute(v, "dp", pairs)


def add(*terms):
    total = terms[0].astype(F32)
    for t in terms[1:]:
        total = total + t.astype(F32)
    return total.astype(BF)


def gather_ring(v, send):
    h = v.shape[0] // 2
    low = send(v, 1)
    high = send(v, -1)
    far_a = send(low[:h], 1)
    far_b = send(high[h:], -1)
    return v, high, far_a, far_b, low


def scatter_ring(own, high, far, low, send):
    h = own.shape[-2] // 2
    r_a = send(far[..., :h, :], -1)
    r_b = send(far[..., h:, :], 1)
    low = add(low, jnp.concatenate([r_a, jnp.zeros_like(r_b)], -2))
    high = add(high, jnp.concatenate([jnp.zeros_like(r_a), r_b], -2))
    from_high = send(low, -1)
    from_low = send(high, 1)
    return own, from_high, from_low


def gather_mp(u):
    h = u.shape[0] // 2
    a = mp_send(u, 1)
    b = mp_send(u, -1)
    z = mp_send(u, 0, 1)
    c_lo = mp_send(a[:h], 1)
    c_hi = mp_send(b[h:], -1)
    za_lo = mp_send(z[:h], 1)
    zb_hi = mp_send(z[h:], -1)
    za_hi = mp_send(a[h:], 0, 1)
    zb_lo = mp_send(b[:h], 0, 1)
    zc_lo = mp_send(za_lo, 1)
    zc_hi = mp_send(zb_hi, -1)
    return [u, b, (c_lo, c_hi), a, z, (zb_lo, zb_hi), (zc_lo, zc_hi), (za_lo, za_hi)]


def scatter_mp(parts):
    own, b, c, a, z, zb, zc, za = parts
    h = own.shape[0] // 2
    r1 = mp_send(zc[:h], -1)
    r2 = mp_send(zc[h:], 1)
    r3 = mp_send(c[:h], -1)
    r5 = mp_send(c[h:], 1)
    r7 = mp_send(za[h:], 0, 1)
    r8 = mp_send(zb[:h], 0, 1)
    r4 = mp_send(add(za[:h], r1), -1)
    r6 = mp_send(add(zb[h:], r2), 1)
    r9 = mp_send(add(a, jnp.concatenate([r3, r7], 0)), -1)
    r10 = mp_send(add(b, jnp.concatenate([r8, r5], 0)), 1)
    r11 = mp_send(add(z, jnp.concatenate([r4, r6], 0)), 0, 1)
    return add(own, r9, r10, r11)


def a2a_dp(v):
    w = v.reshape(32, SLOTS, v.shape[-1])
    return lax.all_to_all(w, "dp", split_axis=0, concat_axis=0, tiled=True).reshape(v.shape)


def expert_kernel(split, *refs):
    n_in = sum(2 if s else 1 for s in split)
    u_refs, g_refs = refs[:n_in], refs[n_in : 2 * n_in]
    gate_ref, up_ref, down_ref = refs[2 * n_in : 2 * n_in + 3]
    outs = refs[2 * n_in + 3 :]
    x_refs, y_refs = outs[: len(split)], outs[len(split) :]
    first_half = pl.program_id(0) < pl.num_programs(0) // 2

    def pieces(rs):
        out, at = [], 0
        for s in split:
            if s:
                out.append(jnp.where(first_half, rs[at][...], rs[at + 1][...]))
                at += 2
            else:
                out.append(rs[at][...])
                at += 1
        return out

    us, gs = pieces(u_refs), pieces(g_refs)
    width = us[0].shape[1] // 2
    nt = (((1,), (1,)), ((), ()))
    nn = (((1,), (0,)), ((), ()))
    xs, ys = [], []
    for e in range(2):
        cut = slice(e * width, (e + 1) * width)
        u = jnp.concatenate([p[:, cut] for p in us], axis=1)
        g = jnp.concatenate([p[:, cut] for p in gs], axis=1)
        a = lax.dot_general(u, gate_ref[e], nt, preferred_element_type=F32)
        b = lax.dot_general(u, up_ref[e], nt, preferred_element_type=F32)
        dz = lax.dot_general(g, down_ref[e], nt, preferred_element_type=F32)
        sig = jax.nn.sigmoid(a)
        silu = a * sig
        z = (silu * b).astype(BF)
        da = (dz * b * sig * (1.0 + a * (1.0 - sig))).astype(BF)
        db = (dz * silu).astype(BF)
        x = lax.dot_general(da, gate_ref[e], nn, preferred_element_type=F32)
        x = x + lax.dot_general(db, up_ref[e], nn, preferred_element_type=F32)
        xs.append(x)
        ys.append(lax.dot_general(z, down_ref[e], nn, preferred_element_type=F32))
    for k in range(len(split)):
        cut = slice(k * width, (k + 1) * width)
        x_refs[k][...] = jnp.concatenate([x[:, cut] for x in xs], axis=1).astype(BF)
        y_refs[k][...] = jnp.concatenate([y[:, cut] for y in ys], axis=1).astype(BF)


def experts(us, gs, gate, up, down):
    rows, width = us[0].shape
    split = tuple(isinstance(u, tuple) for u in us)
    block = rows // 4
    flat, specs = [], []
    for group in (us, gs):
        for p in group:
            if isinstance(p, tuple):
                flat += list(p)
                specs.append(pl.BlockSpec((block, width), lambda r: (jnp.minimum(r, 1), 0)))
                specs.append(pl.BlockSpec((block, width), lambda r: (jnp.maximum(r - 2, 0), 0)))
            else:
                flat.append(p)
                specs.append(pl.BlockSpec((block, width), lambda r: (r, 0)))
    for w in (gate, up, down):
        specs.append(pl.BlockSpec(w.shape, lambda r: (0, 0, 0)))
    n_out = 2 * len(us)
    out = pl.pallas_call(
        lambda *refs: expert_kernel(split, *refs),
        grid=(4,),
        in_specs=specs,
        out_specs=[pl.BlockSpec((block, width), lambda r: (r, 0))] * n_out,
        out_shape=[jax.ShapeDtypeStruct((rows, width), BF)] * n_out,
        compiler_params=pltpu.CompilerParams(vmem_limit_bytes=44 * 1024 * 1024),
        cost_estimate=pl.CostEstimate(
            flops=12 * 2 * rows * 2560 * 192, bytes_accessed=30_000_000, transcendentals=2 * rows * 192
        ),
        name="experts",
    )(*flat, gate, up, down)
    return list(out[: len(us)]), list(out[len(us) :])


def gelu_parts(preact):
    def smooth(values):
        return jax.nn.gelu(values, approximate=True)

    result, pullback = jax.vjp(smooth, preact)
    return (result, pullback(jnp.ones_like(preact))[0])


def adamw_update(weight, gradient, first, second):
    first_new = BETA_ONE * first + (1.0 - BETA_ONE) * gradient
    second_new = BETA_TWO * second + (1.0 - BETA_TWO) * gradient * gradient
    update = first_new / FIRST_FIX / (jnp.sqrt(second_new / SECOND_FIX) + EPSILON)
    current = weight.astype(F32)
    return (
        (current - LEARN_RATE * (update + WEIGHT_DECAY * current)).astype(BF),
        first_new,
        second_new,
    )


def rolled(v, axis, by):
    n = v.shape[axis]
    return lax.dynamic_slice_in_dim(jnp.concatenate([v, v], axis), by, n, axis)


def routing(routes, gate_weights):
    rows = routes.shape[0]
    names = jnp.arange(EXPERTS, dtype=jnp.int32)[:, None]
    hit = jnp.zeros((EXPERTS, rows), F32)
    weight = jnp.zeros((EXPERTS, rows), F32)
    for k in range(TOP):
        same = routes[:, k][None, :] == names
        hit = hit + same.astype(F32)
        weight = weight + jnp.where(same, gate_weights[:, k][None, :], 0.0)
    t = jnp.arange(rows, dtype=jnp.int32)
    before = (t[:, None] < t[None, :]).astype(BF)
    count = jnp.dot(hit.astype(BF), before, preferred_element_type=F32)
    place = jnp.where(hit > 0.0, count, -1.0)
    slots = jnp.arange(SLOTS, dtype=F32)[None, :, None]
    chosen, weighted = [], []
    for e in range(2):
        sel = place.reshape(EXPERTS // 2, 2, rows)[:, e][:, None, :] == slots
        w = weight.reshape(EXPERTS // 2, 2, rows)[:, e][:, None, :]
        chosen.append(sel.astype(BF).reshape(-1, rows))
        weighted.append(jnp.where(sel, w, 0.0).reshape(-1, rows))
    return chosen, weighted


def over_slots(sel, v, precision=None):
    return lax.dot_general(
        sel, v, (((0,), (0,)), ((), ())), precision=precision, preferred_element_type=F32
    )


def local(
    features,
    proj_in,
    proj_out,
    expert_gate,
    expert_up,
    expert_down,
    routes,
    gate_weights,
    cotangent,
    first_in,
    second_in,
    first_out,
    second_out,
):
    rows, model_width = cotangent.shape
    i = lax.axis_index("dp")
    j = lax.axis_index("mp")
    dz, dy, dc = i // (RY * 2), i // 2 % RY, i % 2
    mz, mx = j // NX, j % NX
    width = model_width // (NX * NZ)
    vis = features.shape[1] // 32
    hid = proj_out.shape[0]

    feats = features.T.reshape(RZ, RY, 2, vis, rows)
    feats = rolled(rolled(rolled(feats, 0, dz), 1, dy), 2, dc)
    feats = jnp.transpose(feats, (2, 1, 0, 3, 4)).reshape(-1, rows)

    own, high, far_a, far_b, low = gather_ring(proj_in, lambda v, k: dp_send(v, dz=k))
    column = jnp.concatenate([own, high, far_a, far_b, low], 0)
    plane = gather_ring(column, lambda v, k: dp_send(v, dy=k))
    other = [dp_send(p, dc=1) for p in plane]
    weights_in = jnp.concatenate(list(plane) + other, 0)

    chosen, weighted = routing(routes, gate_weights)
    cot_cols = lax.dynamic_slice_in_dim(cotangent, j * width, width, 1)

    def picked_grads(e):
        w = jnp.sum(weighted[e], axis=1, keepdims=True)
        return (w * jnp.dot(chosen[e], cot_cols, preferred_element_type=F32)).astype(BF)

    send_grads = jnp.concatenate([picked_grads(0), picked_grads(1)], 1)
    grad_parts = gather_mp(a2a_dp(send_grads))

    def arranged(w):
        w = w.reshape(2, w.shape[1], NZ, NX * width)
        w = rolled(w, 2, mz)
        return rolled(w.reshape(2, -1, NX * width), 2, mx * width).reshape(2, -1, model_width)

    gate = arranged(jnp.swapaxes(expert_gate, 1, 2))
    up = arranged(jnp.swapaxes(expert_up, 1, 2))
    down = arranged(expert_down)

    preact = lax.dot_general(
        feats, weights_in, (((0,), (0,)), ((), ())), preferred_element_type=F32
    )
    activated, gelu_slope = gelu_parts(preact)
    hidden = activated.astype(BF)
    partial_value = jnp.dot(hidden, proj_out, preferred_element_type=F32).astype(BF)
    pieces = jnp.moveaxis(partial_value.reshape(rows, NX * NZ, width), 1, 0)
    arrived = lax.all_to_all(pieces, "mp", split_axis=0, concat_axis=0, tiled=True)
    mapped_cols = jnp.sum(arrived.astype(F32), axis=0).astype(BF)

    send_rows = jnp.concatenate(
        [jnp.dot(chosen[e], mapped_cols, preferred_element_type=F32).astype(BF) for e in range(2)],
        1,
    )
    row_parts = gather_mp(a2a_dp(send_rows))

    x_parts, y_parts = experts(row_parts, grad_parts, gate, up, down)
    x_sum = scatter_mp(x_parts)
    *y_parts, x_sum = lax.optimization_barrier((*y_parts, x_sum))
    y_sum = scatter_mp(y_parts)

    back_in = a2a_dp(x_sum)
    grad_cols = (
        cot_cols.astype(F32)
        + over_slots(chosen[0], back_in[:, :width])
        + over_slots(chosen[1], back_in[:, width:])
    ).astype(BF)

    def all_columns(cols):
        same = jnp.broadcast_to(cols[None], (NX * NZ,) + cols.shape)
        got = lax.all_to_all(same, "mp", split_axis=0, concat_axis=0, tiled=True)
        return jnp.moveaxis(got, 0, 1).reshape(rows, model_width)

    grad_mapped = all_columns(grad_cols)
    grad_hidden = lax.dot_general(
        grad_mapped, proj_out, (((1,), (1,)), ((), ())), preferred_element_type=F32
    )
    grad_pre = (grad_hidden * gelu_slope).astype(BF)
    out_part = model_width // 32
    term_in = jnp.einsum(
        "tnv,th->nvh", features.reshape(rows, 32, vis), grad_pre, preferred_element_type=F32
    )
    term_out = jnp.einsum(
        "tnd,th->ndh", grad_mapped.reshape(rows, 32, out_part), hidden, preferred_element_type=F32
    )
    share = vis + out_part
    terms = jnp.concatenate([term_in, term_out], 1).astype(BF).reshape(RZ, RY, 2, share, hid)

    def at(v, axis, k):
        return lax.dynamic_index_in_dim(v, k, axis, keepdims=False)

    kept = at(terms, 2, dc)
    total = add(kept, dp_send(at(terms, 2, 1 - dc), dc=1))
    total = add(
        *scatter_ring(
            *(at(total, 1, (dy + k) % RY) for k in range(4)), lambda v, k: dp_send(v, dy=k)
        )
    )
    shares = sum(
        t.astype(F32)
        for t in scatter_ring(
            *(at(total, 0, (dz + k) % RZ) for k in range(4)), lambda v, k: dp_send(v, dz=k)
        )
    )
    grad_in = shares[:vis]
    grad_out = shares[vis:].T

    back_out = a2a_dp(y_sum)
    moe_cols = (
        mapped_cols.astype(F32)
        + over_slots(weighted[0], back_out[:, :width].astype(F32), lax.Precision.HIGHEST)
        + over_slots(weighted[1], back_out[:, width:].astype(F32), lax.Precision.HIGHEST)
    ).astype(BF)
    moe_out = all_columns(moe_cols)

    own_out = lax.dynamic_slice_in_dim(proj_out, i * out_part, out_part, 1)
    new_in, first_in_new, second_in_new = adamw_update(proj_in, grad_in, first_in, second_in)
    new_out, first_out_new, second_out_new = adamw_update(own_out, grad_out, first_out, second_out)
    return (moe_out, new_in, new_out, first_in_new, second_in_new, first_out_new, second_out_new)


def solution(mesh):
    return jax.shard_map(
        local,
        mesh=mesh,
        in_specs=(
            P("dp", None),
            P("dp", "mp"),
            P("mp", None),
            P("dp", None, "mp"),
            P("dp", None, "mp"),
            P("dp", "mp", None),
            P("dp", None),
            P("dp", None),
            P("dp", None),
            P("dp", "mp"),
            P("dp", "mp"),
            P("mp", "dp"),
            P("mp", "dp"),
        ),
        out_specs=(
            P("dp", None),
            P("dp", "mp"),
            P("mp", "dp"),
            P("dp", "mp"),
            P("dp", "mp"),
            P("mp", "dp"),
            P("mp", "dp"),
        ),
        check_vma=False,
    )
```

```python
import jax
import jax.numpy as jnp
from jax import lax
from jax.experimental import pallas as pl
from jax.experimental.pallas import tpu as pltpu
from jax.sharding import PartitionSpec as P

EXPERTS = 64
TOP = 6
SLOTS = 16
NX, NZ = 4, 2
RY, RZ = 4, 4

BETA_ONE = 0.9
BETA_TWO = 0.999
EPSILON = 1e-08
LEARN_RATE = 0.001
WEIGHT_DECAY = 0.1
FIRST_FIX = 1.0 - 0.9**50 * 0.9**50
SECOND_FIX = 1.0 - 0.999**50 * 0.999**50

BF = jnp.bfloat16
F32 = jnp.float32


def mp_send(v, dx, dz=0):
    pairs = [
        (z * NX + x, (z + dz) % NZ * NX + (x + dx) % NX) for z in range(NZ) for x in range(NX)
    ]
    return lax.ppermute(v, "mp", pairs)


def dp_send(v, dz=0, dy=0, dc=0):
    pairs = [
        ((z * RY + y) * 2 + c, ((z + dz) % RZ * RY + (y + dy) % RY) * 2 + (c + dc) % 2)
        for z in range(RZ)
        for y in range(RY)
        for c in range(2)
    ]
    return lax.ppermute(v, "dp", pairs)


def add(*terms):
    total = terms[0].astype(F32)
    for t in terms[1:]:
        total = total + t.astype(F32)
    return total.astype(BF)


def gather_ring(v, send):
    h = v.shape[0] // 2
    low = send(v, 1)
    high = send(v, -1)
    far_a = send(low[:h], 1)
    far_b = send(high[h:], -1)
    return v, high, far_a, far_b, low


def scatter_ring(own, high, far, low, send):
    h = own.shape[-2] // 2
    high_a, high_b = high[..., :h, :], high[..., h:, :]
    low_a, low_b = low[..., :h, :], low[..., h:, :]
    r_a = send(far[..., :h, :], -1)
    r_b = send(far[..., h:, :], 1)
    s_b = send(low_b, -1)
    s_a = send(high_a, 1)
    t_a = send(add(low_a, r_a), -1)
    t_b = send(add(high_b, r_b), 1)
    return jnp.concatenate(
        [
            own[..., :h, :].astype(F32) + s_a.astype(F32) + t_a.astype(F32),
            own[..., h:, :].astype(F32) + s_b.astype(F32) + t_b.astype(F32),
        ],
        -2,
    )


def gather_near(u):
    return mp_send(u, 1), mp_send(u, -1), mp_send(u, 0, 1)


def gather_far(u, a, b, z):
    h = u.shape[0] // 2
    c_lo = mp_send(a[:h], 1)
    c_hi = mp_send(b[h:], -1)
    za_lo = mp_send(z[:h], 1)
    zb_hi = mp_send(z[h:], -1)
    za_hi = mp_send(a[h:], 0, 1)
    zb_lo = mp_send(b[:h], 0, 1)
    zc_lo = mp_send(za_lo, 1)
    zc_hi = mp_send(zb_hi, -1)
    return [u, b, (c_lo, c_hi), a, z, (zb_lo, zb_hi), (zc_lo, zc_hi), (za_lo, za_hi)]


def scatter_far(parts):
    own, b, c, a, z, zb, zc, za = parts
    h = own.shape[0] // 2
    return (
        mp_send(zc[:h], -1),
        mp_send(zc[h:], 1),
        mp_send(c[:h], -1),
        mp_send(c[h:], 1),
        mp_send(za[h:], 0, 1),
        mp_send(zb[:h], 0, 1),
    )


def scatter_near(parts, far):
    own, b, c, a, z, zb, zc, za = parts
    r1, r2, r3, r5, r7, r8 = far
    h = own.shape[0] // 2
    r4 = mp_send(add(za[:h], r1), -1)
    r6 = mp_send(add(zb[h:], r2), 1)
    r9 = mp_send(add(a, jnp.concatenate([r3, r7], 0)), -1)
    r10 = mp_send(add(b, jnp.concatenate([r8, r5], 0)), 1)
    r11 = mp_send(add(z, jnp.concatenate([r4, r6], 0)), 0, 1)
    return add(own, r9, r10, r11)


def a2a_dp(v):
    w = v.reshape(32, SLOTS, v.shape[-1])
    return lax.all_to_all(w, "dp", split_axis=0, concat_axis=0, tiled=True).reshape(v.shape)


NT = (((1,), (1,)), ((), ()))
NN = (((1,), (0,)), ((), ()))
MIB = 1024 * 1024


def dot(x, y, dims):
    return lax.dot_general(x, y, dims, preferred_element_type=F32)


def piece_specs(pieces, block):
    flat, specs = [], []
    for p in pieces:
        if isinstance(p, tuple):
            flat += list(p)
            width = p[0].shape[1]
            specs.append(pl.BlockSpec((block, width), lambda r: (jnp.minimum(r, 1), 0)))
            specs.append(pl.BlockSpec((block, width), lambda r: (jnp.maximum(r - 2, 0), 0)))
        else:
            flat.append(p)
            specs.append(pl.BlockSpec((block, p.shape[1]), lambda r: (r, 0)))
    return flat, specs


def piece_values(split, refs):
    first_half = pl.program_id(0) < 2
    out, at = [], 0
    for s in split:
        if s:
            out.append(jnp.where(first_half, refs[at][...], refs[at + 1][...]))
            at += 2
        else:
            out.append(refs[at][...])
            at += 1
    return out


def whole(w):
    return pl.BlockSpec(w.shape, lambda r: (0,) * w.ndim)


def arrange_kernel(place_ref, *refs):
    mz, mx = place_ref[0], place_ref[1]
    for src, dst in zip(refs[:3], refs[3:]):
        half = src.shape[2] // NZ
        step = half // NX
        for k in range(NZ):
            at = pl.multiple_of(lax.rem(mz + k, NZ) * half, half)
            v = src[0, :, pl.ds(at, half)]
            for x in range(NX):

                @pl.when(mx == x)
                def _(v=v, x=x, k=k, dst=dst):
                    turned = v if x == 0 else jnp.concatenate([v[:, x * step :], v[:, : x * step]], 1)
                    dst[0, :, k * half : (k + 1) * half] = turned


def arranged(place, *ws):
    spec = pl.BlockSpec((1,) + ws[0].shape[1:], lambda e, p: (e, 0, 0))
    return pl.pallas_call(
        arrange_kernel,
        grid_spec=pltpu.PrefetchScalarGridSpec(
            num_scalar_prefetch=1, grid=(2,), in_specs=[spec] * 3, out_specs=[spec] * 3
        ),
        out_shape=[jax.ShapeDtypeStruct(w.shape, BF) for w in ws],
        compiler_params=pltpu.CompilerParams(vmem_limit_bytes=24 * MIB),
        cost_estimate=pl.CostEstimate(flops=8_000_000, bytes_accessed=12_000_000, transcendentals=0),
        name="arrange",
    )(place, *ws)


def by_expert(pieces, e):
    width = pieces[0].shape[1] // 2
    return jnp.concatenate([p[:, e * width : (e + 1) * width] for p in pieces], axis=1)


def grads_kernel(split, *refs):
    down_ref, dz_ref = refs[-2:]
    gs = piece_values(split, refs[:-2])
    for e in range(2):
        dz_ref[e] = dot(by_expert(gs, e), down_ref[e], NT)


def expert_grads(gs, down):
    flat, specs = piece_specs(gs, 128)
    rows, hidden = gs[0].shape[0], down.shape[1]
    return pl.pallas_call(
        lambda *refs: grads_kernel([isinstance(g, tuple) for g in gs], *refs),
        grid=(4,),
        in_specs=specs + [whole(down)],
        out_specs=pl.BlockSpec((2, 128, hidden), lambda r: (0, r, 0)),
        out_shape=jax.ShapeDtypeStruct((2, rows, hidden), F32),
        compiler_params=pltpu.CompilerParams(vmem_limit_bytes=24 * MIB),
        cost_estimate=pl.CostEstimate(flops=1_000_000_000, bytes_accessed=8_000_000, transcendentals=0),
        name="expert_grads",
    )(*flat, down)


def rows_kernel(split, n_in, *refs):
    gate_ref, up_ref, dz_ref, z_ref = refs[n_in : n_in + 4]
    x_refs = refs[n_in + 4 :]
    us = piece_values(split, refs[:n_in])
    xs = []
    for e in range(2):
        u = by_expert(us, e)
        a = dot(u, gate_ref[e], NT)
        b = dot(u, up_ref[e], NT)
        dz = dz_ref[e]
        sig = jax.nn.sigmoid(a)
        silu = a * sig
        z_ref[e] = (silu * b).astype(BF)
        da = (dz * b * sig * (1.0 + a * (1.0 - sig))).astype(BF)
        db = (dz * silu).astype(BF)
        xs.append(dot(da, gate_ref[e], NN) + dot(db, up_ref[e], NN))
    width = us[0].shape[1] // 2
    for k, ref in enumerate(x_refs):
        cut = slice(k * width, (k + 1) * width)
        ref[...] = jnp.concatenate([x[:, cut] for x in xs], axis=1).astype(BF)


def expert_rows(us, gate, up, dz):
    flat, specs = piece_specs(us, 128)
    rows, width = us[0].shape
    hidden = gate.shape[1]
    part = pl.BlockSpec((2, 128, hidden), lambda r: (0, r, 0))
    out = pl.pallas_call(
        lambda *refs: rows_kernel([isinstance(u, tuple) for u in us], len(flat), *refs),
        grid=(4,),
        in_specs=specs + [whole(gate), whole(up), part],
        out_specs=[part] + [pl.BlockSpec((128, width), lambda r: (r, 0))] * len(us),
        out_shape=[jax.ShapeDtypeStruct((2, rows, hidden), BF)]
        + [jax.ShapeDtypeStruct((rows, width), BF)] * len(us),
        compiler_params=pltpu.CompilerParams(vmem_limit_bytes=32 * MIB),
        cost_estimate=pl.CostEstimate(flops=4_000_000_000, bytes_accessed=15_000_000, transcendentals=200_000),
        name="expert_rows",
    )(*flat, gate, up, dz)
    return out[0], list(out[1:])


def outs_kernel(z_ref, down_ref, *y_refs):
    ys = [dot(z_ref[e], down_ref[e], NN) for e in range(2)]
    width = y_refs[0].shape[1] // 2
    for k, ref in enumerate(y_refs):
        cut = slice(k * width, (k + 1) * width)
        ref[...] = jnp.concatenate([y[:, cut] for y in ys], axis=1).astype(BF)


def expert_outs(z, down, count):
    rows = z.shape[1]
    width = 2 * down.shape[2] // count
    return list(
        pl.pallas_call(
            outs_kernel,
            grid=(4,),
            in_specs=[pl.BlockSpec((2, 128, z.shape[2]), lambda r: (0, r, 0)), whole(down)],
            out_specs=[pl.BlockSpec((128, width), lambda r: (r, 0))] * count,
            out_shape=[jax.ShapeDtypeStruct((rows, width), BF)] * count,
            compiler_params=pltpu.CompilerParams(vmem_limit_bytes=24 * MIB),
            cost_estimate=pl.CostEstimate(flops=1_000_000_000, bytes_accessed=8_000_000, transcendentals=0),
            name="expert_outs",
        )(z, down)
    )


def block_terms(d, feats_ref, turned_ref, pre, hidden):
    vis, out_part = feats_ref.shape[0] // 32, turned_ref.shape[0] // 32
    term_in = dot(feats_ref[pl.ds(pl.multiple_of(d * vis, 16), vis), :], pre, NT)
    term_out = dot(turned_ref[pl.ds(pl.multiple_of(d * out_part, 16), out_part), :], hidden, NT)
    both = jnp.concatenate([term_in, term_out], axis=0)
    h = both.shape[0] // 2
    return jnp.concatenate([both[:h], both[h:]], axis=1).astype(BF)


def sent_kernel(place_ref, turned_ref, w_ref, slope_ref, hidden_ref, feats_ref, pre_ref, out_ref):
    z = pl.program_id(0)
    dz, dy, dc = place_ref[0], place_ref[1], place_ref[2]

    @pl.when(z == 0)
    def _():
        pre_ref[...] = (dot(w_ref[...], turned_ref[...], NN) * slope_ref[...]).astype(BF)

    for y in range(RY):
        d = (lax.rem(dz + z, RZ) * RY + lax.rem(dy + y, RY)) * 2 + (1 - dc)
        out_ref[y, 0] = block_terms(d, feats_ref, turned_ref, pre_ref[...], hidden_ref[...])


def kept_kernel(place_ref, pre_ref, turned_ref, hidden_ref, feats_ref, got_ref, *out_refs):
    z = pl.program_id(0)
    dz, dy, dc = place_ref[0], place_ref[1], place_ref[2]
    for y in range(RY):
        d = (lax.rem(dz + z, RZ) * RY + lax.rem(dy + y, RY)) * 2 + dc
        terms = block_terms(d, feats_ref, turned_ref, pre_ref[...], hidden_ref[...])
        out_refs[y][0] = (terms.astype(F32) + got_ref[y, 0].astype(F32)).astype(BF)


def sent_terms(place, turned, proj_out, slope, hidden, feats):
    hid, rows = hidden.shape
    share = (feats.shape[0] + proj_out.shape[1]) // 32

    def full(w):
        return pl.BlockSpec(w.shape, lambda r, p: (0,) * w.ndim)

    pre = jax.ShapeDtypeStruct((hid, rows), BF)
    shape = (RY, RZ, share // 2, 2 * hid)
    return pl.pallas_call(
        sent_kernel,
        grid_spec=pltpu.PrefetchScalarGridSpec(
            num_scalar_prefetch=1,
            grid=(RZ,),
            in_specs=[full(turned), full(proj_out), full(slope), full(hidden), full(feats)],
            out_specs=[full(pre), pl.BlockSpec((RY, 1) + shape[2:], lambda r, p: (0, r, 0, 0))],
        ),
        out_shape=[pre, jax.ShapeDtypeStruct(shape, BF)],
        compiler_params=pltpu.CompilerParams(vmem_limit_bytes=24 * MIB),
        cost_estimate=pl.CostEstimate(flops=600_000_000, bytes_accessed=7_000_000, transcendentals=0),
        name="sent_terms",
    )(place, turned, proj_out, slope, hidden, feats)


def kept_terms(place, pre, turned, hidden, feats, got):
    def full(w):
        return pl.BlockSpec(w.shape, lambda r, p: (0,) * w.ndim)

    share, hid = got.shape[2:]
    return pl.pallas_call(
        kept_kernel,
        grid_spec=pltpu.PrefetchScalarGridSpec(
            num_scalar_prefetch=1,
            grid=(RZ,),
            in_specs=[full(pre), full(turned), full(hidden), full(feats)]
            + [pl.BlockSpec((RY, 1, share, hid), lambda r, p: (0, r, 0, 0))],
            out_specs=[pl.BlockSpec((1, share, hid), lambda r, p: (r, 0, 0))] * RY,
        ),
        out_shape=[jax.ShapeDtypeStruct((RZ, share, hid), BF)] * RY,
        compiler_params=pltpu.CompilerParams(vmem_limit_bytes=24 * MIB),
        cost_estimate=pl.CostEstimate(flops=400_000_000, bytes_accessed=7_000_000, transcendentals=0),
        name="kept_terms",
    )(place, pre, turned, hidden, feats, got)


def tied(first, *others):
    return lax.optimization_barrier((first, *others))[0]


def gelu_parts(preact):
    def smooth(values):
        return jax.nn.gelu(values, approximate=True)

    result, pullback = jax.vjp(smooth, preact)
    return (result, pullback(jnp.ones_like(preact))[0])


def adamw_update(weight, gradient, first, second):
    first_new = BETA_ONE * first + (1.0 - BETA_ONE) * gradient
    second_new = BETA_TWO * second + (1.0 - BETA_TWO) * gradient * gradient
    update = first_new / FIRST_FIX / (jnp.sqrt(second_new / SECOND_FIX) + EPSILON)
    current = weight.astype(F32)
    return (
        (current - LEARN_RATE * (update + WEIGHT_DECAY * current)).astype(BF),
        first_new,
        second_new,
    )


def rolled(v, axis, by):
    n = v.shape[axis]
    return lax.dynamic_slice_in_dim(jnp.concatenate([v, v], axis), by, n, axis)


def routing(routes, gate_weights):
    rows = routes.shape[0]
    names = jnp.arange(EXPERTS, dtype=jnp.int32)[:, None]
    hit = jnp.zeros((EXPERTS, rows), F32)
    weight = jnp.zeros((EXPERTS, rows), F32)
    for k in range(TOP):
        same = routes[:, k][None, :] == names
        hit = hit + same.astype(F32)
        weight = weight + jnp.where(same, gate_weights[:, k][None, :], 0.0)
    t = jnp.arange(rows, dtype=jnp.int32)
    before = (t[:, None] < t[None, :]).astype(BF)
    count = jnp.dot(hit.astype(BF), before, preferred_element_type=F32)
    place = jnp.where(hit > 0.0, count, -1.0)
    slots = jnp.arange(SLOTS, dtype=F32)[None, :, None]
    chosen, weighted = [], []
    for e in range(2):
        sel = place.reshape(EXPERTS // 2, 2, rows)[:, e][:, None, :] == slots
        w = weight.reshape(EXPERTS // 2, 2, rows)[:, e][:, None, :]
        chosen.append(sel.astype(BF).reshape(-1, rows))
        weighted.append(jnp.where(sel, w, 0.0).reshape(-1, rows))
    return chosen, weighted


def over_slots(v, sel, precision=None):
    return lax.dot_general(
        v, sel, (((0,), (0,)), ((), ())), precision=precision, preferred_element_type=F32
    )


def local(
    features,
    proj_in,
    proj_out,
    expert_gate,
    expert_up,
    expert_down,
    routes,
    gate_weights,
    cotangent,
    first_in,
    second_in,
    first_out,
    second_out,
):
    rows, model_width = cotangent.shape
    i = lax.axis_index("dp")
    j = lax.axis_index("mp")
    dz, dy, dc = i // (RY * 2), i // 2 % RY, i % 2
    mz, mx = j // NX, j % NX
    width = model_width // (NX * NZ)
    vis = features.shape[1] // 32

    turned_feats = features.T
    feats = turned_feats.reshape(RZ, RY, 2, vis, rows)
    feats = rolled(rolled(rolled(feats, 0, dz), 1, dy), 2, dc)
    feats = jnp.transpose(feats, (2, 1, 0, 3, 4)).reshape(-1, rows)

    own, high, far_a, far_b, low = gather_ring(proj_in, lambda v, k: dp_send(v, dz=k))
    column = jnp.concatenate([own, high, far_a, far_b, low], 0)
    column, gate, up, down = lax.optimization_barrier(
        (
            column,
            *arranged(
                jnp.stack([mz, mx]).astype(jnp.int32),
                jnp.swapaxes(expert_gate, 1, 2),
                jnp.swapaxes(expert_up, 1, 2),
                expert_down,
            ),
        )
    )
    plane = gather_ring(column, lambda v, k: dp_send(v, dy=k))
    other = [dp_send(p, dc=1) for p in plane]
    weights_in = jnp.concatenate(list(plane) + other, 0)

    chosen, weighted = routing(routes, gate_weights)
    cot_cols = lax.dynamic_slice_in_dim(cotangent, j * width, width, 1)

    def picked_grads(e):
        w = jnp.sum(weighted[e], axis=1, keepdims=True)
        return (w * jnp.dot(chosen[e], cot_cols, preferred_element_type=F32)).astype(BF)

    send_grads = jnp.concatenate([picked_grads(0), picked_grads(1)], 1)
    own_grads = a2a_dp(tied(send_grads, plane[1], plane[4]))

    preact = lax.dot_general(
        weights_in, feats, (((0,), (0,)), ((), ())), preferred_element_type=F32
    )
    activated, gelu_slope = gelu_parts(preact)
    hidden = activated.astype(BF)
    partial_value = lax.dot_general(
        proj_out, hidden, (((0,), (0,)), ((), ())), preferred_element_type=F32
    ).astype(BF)
    partial_value, own_grads = lax.optimization_barrier((partial_value, own_grads))
    near_grads = gather_near(own_grads)
    arrived = lax.all_to_all(
        partial_value.reshape(NX * NZ, width, rows), "mp", split_axis=0, concat_axis=0, tiled=True
    )
    mapped_cols = jnp.sum(arrived.astype(F32), axis=0).astype(BF)

    send_rows = jnp.concatenate([dot(chosen[e], mapped_cols, NT).astype(BF) for e in range(2)], 1)
    grad_parts = gather_far(own_grads, *near_grads)
    own_rows = a2a_dp(send_rows)
    leaves, tree = jax.tree.flatten(grad_parts)
    own_rows, *leaves = lax.optimization_barrier((own_rows, *leaves))
    grad_parts = jax.tree.unflatten(tree, leaves)
    near_rows = gather_near(own_rows)
    inner_grads = expert_grads(grad_parts, down)
    inner_grads, *near_rows = lax.optimization_barrier((inner_grads, *near_rows))
    row_parts = gather_far(own_rows, *near_rows)

    inner, x_parts = expert_rows(row_parts, gate, up, inner_grads)
    y_parts = expert_outs(inner, down, len(x_parts))
    x_sum = scatter_near(x_parts, scatter_far(x_parts))
    *y_parts, x_sum = lax.optimization_barrier((*y_parts, x_sum))
    y_sum = scatter_near(y_parts, scatter_far(y_parts))

    back_in = a2a_dp(x_sum)
    grad_cols = (
        cot_cols.T.astype(F32)
        + over_slots(back_in[:, :width], chosen[0])
        + over_slots(back_in[:, width:], chosen[1])
    ).astype(BF)

    def by_columns(cols):
        same = jnp.broadcast_to(cols[None], (NX * NZ,) + cols.shape)
        got = lax.all_to_all(same, "mp", split_axis=0, concat_axis=0, tiled=True)
        return got.reshape(model_width, rows)

    place = jnp.stack([dz, dy, dc]).astype(jnp.int32)
    turned, y_sum = lax.optimization_barrier((by_columns(grad_cols), y_sum))
    back_out = a2a_dp(y_sum)
    pre, sent = sent_terms(place, turned, proj_out, gelu_slope, hidden, turned_feats)
    got = dp_send(sent, dc=1)
    total = kept_terms(place, pre, turned, hidden, turned_feats, got)
    total = scatter_ring(*total, lambda v, k: dp_send(v, dy=k)).astype(BF)
    total, back_out = lax.optimization_barrier((total, back_out))
    shares = scatter_ring(*(total[k] for k in range(RZ)), lambda v, k: dp_send(v, dz=k))
    shares = jnp.concatenate([shares[:, : shares.shape[1] // 2], shares[:, shares.shape[1] // 2 :]], 0)
    grad_in = shares[:vis]
    grad_out = shares[vis:].T

    moe_cols = (
        mapped_cols.astype(F32)
        + over_slots(back_out[:, :width].astype(F32), weighted[0], lax.Precision.HIGHEST)
        + over_slots(back_out[:, width:].astype(F32), weighted[1], lax.Precision.HIGHEST)
    ).astype(BF)
    moe_out = by_columns(moe_cols).T

    out_part = model_width // 32
    own_out = lax.dynamic_slice_in_dim(proj_out, i * out_part, out_part, 1)
    new_in, first_in_new, second_in_new = adamw_update(proj_in, grad_in, first_in, second_in)
    new_out, first_out_new, second_out_new = adamw_update(own_out, grad_out, first_out, second_out)
    return (moe_out, new_in, new_out, first_in_new, second_in_new, first_out_new, second_out_new)


def solution(mesh):
    return jax.shard_map(
        local,
        mesh=mesh,
        in_specs=(
            P("dp", None),
            P("dp", "mp"),
            P("mp", None),
            P("dp", None, "mp"),
            P("dp", None, "mp"),
            P("dp", "mp", None),
            P("dp", None),
            P("dp", None),
            P("dp", None),
            P("dp", "mp"),
            P("dp", "mp"),
            P("mp", "dp"),
            P("mp", "dp"),
        ),
        out_specs=(
            P("dp", None),
            P("dp", "mp"),
            P("mp", "dp"),
            P("dp", "mp"),
            P("dp", "mp"),
            P("mp", "dp"),
            P("mp", "dp"),
        ),
        check_vma=False,
    )
```

```python
import jax
import jax.numpy as jnp
from jax import lax
from jax.experimental import pallas as pl
from jax.experimental.pallas import tpu as pltpu
from jax.sharding import PartitionSpec as P

EXPERTS = 64
TOP = 6
SLOTS = 16
NX, NZ = 4, 2
RY, RZ = 4, 4

BETA_ONE = 0.9
BETA_TWO = 0.999
EPSILON = 1e-08
LEARN_RATE = 0.001
WEIGHT_DECAY = 0.1
FIRST_FIX = 1.0 - 0.9**50 * 0.9**50
SECOND_FIX = 1.0 - 0.999**50 * 0.999**50

BF = jnp.bfloat16
F32 = jnp.float32


def mp_send(v, dx, dz=0):
    pairs = [
        (z * NX + x, (z + dz) % NZ * NX + (x + dx) % NX) for z in range(NZ) for x in range(NX)
    ]
    return lax.ppermute(v, "mp", pairs)


def dp_send(v, dz=0, dy=0, dc=0):
    pairs = [
        ((z * RY + y) * 2 + c, ((z + dz) % RZ * RY + (y + dy) % RY) * 2 + (c + dc) % 2)
        for z in range(RZ)
        for y in range(RY)
        for c in range(2)
    ]
    return lax.ppermute(v, "dp", pairs)


def add32(*terms):
    total = terms[0].astype(F32)
    for t in terms[1:]:
        total = total + t.astype(F32)
    return total


def add(*terms):
    return add32(*terms).astype(BF)


def gather_ring(v, send):
    h = v.shape[0] // 2
    low = send(v, 1)
    high = send(v, -1)
    far_a = send(low[:h], 1)
    far_b = send(high[h:], -1)
    return v, high, far_a, far_b, low


def joined(x, y):
    return jnp.concatenate([x, y], -2)


def scatter_end(own, near, got, send):
    from_high, from_low = got
    h = own.shape[-2] // 2
    t_a = send(add(near[..., :h, :], from_high[..., :h, :]), -1)
    t_b = send(add(near[..., h:, :], from_low[..., :h, :]), 1)
    return add32(own, joined(from_low[..., h:, :], from_high[..., h:, :]), joined(t_a, t_b))


def scatter_ring(own, high, far, low, send):
    h = own.shape[-2] // 2
    got = (
        send(joined(far[..., :h, :], low[..., h:, :]), -1),
        send(joined(far[..., h:, :], high[..., :h, :]), 1),
    )
    return scatter_end(own, joined(low[..., :h, :], high[..., h:, :]), got, send)


def gather_near(u):
    return mp_send(u, 1), mp_send(u, -1), mp_send(u, 0, 1)


def gather_far(u, a, b, z):
    h = u.shape[0] // 2
    plus = mp_send(joined(a[:h], z[:h]), 1)
    minus = mp_send(joined(z[h:], b[h:]), -1)
    cross = mp_send(joined(b[:h], a[h:]), 0, 1)
    last_lo = mp_send(plus[h:], 1)
    last_hi = mp_send(minus[:h], -1)
    return [u, a, b, z, plus, minus, cross, last_lo, last_hi]


def piece_order(u, a, b, z, plus, minus, cross, last_lo, last_hi):
    return [
        u,
        b,
        ((plus, 0), (minus, 2)),
        a,
        z,
        ((cross, 0), (minus, 0)),
        ((last_lo, 0), (last_hi, 0)),
        ((plus, 2), (cross, 2)),
    ]


def scatter_far(parts):
    own, b, a, z, minus, plus, cross, near = parts
    return mp_send(minus, -1), mp_send(plus, 1), mp_send(cross, 0, 1)


def scatter_near(parts, far):
    own, b, a, z, minus, plus, cross, near = parts
    g_minus, g_plus, g_cross = far
    h = own.shape[0] // 2
    r4 = mp_send(add(near[:h], g_minus[0]), -1)
    r6 = mp_send(add(near[h:], g_plus[0]), 1)
    r9 = mp_send(add(a, joined(g_minus[1], g_cross[h:])), -1)
    r10 = mp_send(add(b, joined(g_cross[:h], g_plus[1])), 1)
    r11 = mp_send(add(z, joined(r4, r6)), 0, 1)
    return add(own, r9, r10, r11)


def a2a_dp(v):
    w = v.reshape(32, SLOTS, v.shape[-1])
    return lax.all_to_all(w, "dp", split_axis=0, concat_axis=0, tiled=True).reshape(v.shape)


NT = (((1,), (1,)), ((), ()))
NN = (((1,), (0,)), ((), ()))
MIB = 1024 * 1024


def dot(x, y, dims):
    return lax.dot_general(x, y, dims, preferred_element_type=F32)


def piece_specs(pieces, block):
    flat, specs = [], []
    for p in pieces:
        if isinstance(p, tuple):
            (low, i), (high, k) = p
            flat += [low, high]
            shape = (block, low.shape[1])
            specs.append(pl.BlockSpec(shape, lambda r, i=i: (jnp.minimum(r, 1) + i, 0)))
            specs.append(pl.BlockSpec(shape, lambda r, k=k: (jnp.maximum(r - 2, 0) + k, 0)))
        else:
            flat.append(p)
            specs.append(pl.BlockSpec((block, p.shape[1]), lambda r: (r, 0)))
    return flat, specs


def piece_values(split, refs):
    first_half = pl.program_id(0) < 2
    out, at = [], 0
    for s in split:
        if s:
            out.append(jnp.where(first_half, refs[at][...], refs[at + 1][...]))
            at += 2
        else:
            out.append(refs[at][...])
            at += 1
    return out


def whole(w):
    return pl.BlockSpec(w.shape, lambda r: (0,) * w.ndim)


def arrange_kernel(place_ref, *refs):
    mz, mx = place_ref[0], place_ref[1]
    for src, dst in zip(refs[:3], refs[3:]):
        half = src.shape[2] // NZ
        step = half // NX
        for k in range(NZ):
            at = pl.multiple_of(lax.rem(mz + k, NZ) * half, half)
            v = src[0, :, pl.ds(at, half)]
            for x in range(NX):

                @pl.when(mx == x)
                def _(v=v, x=x, k=k, dst=dst):
                    turned = v if x == 0 else jnp.concatenate([v[:, x * step :], v[:, : x * step]], 1)
                    dst[0, :, k * half : (k + 1) * half] = turned


def arranged(place, *ws):
    spec = pl.BlockSpec((1,) + ws[0].shape[1:], lambda e, p: (e, 0, 0))
    return pl.pallas_call(
        arrange_kernel,
        grid_spec=pltpu.PrefetchScalarGridSpec(
            num_scalar_prefetch=1, grid=(2,), in_specs=[spec] * 3, out_specs=[spec] * 3
        ),
        out_shape=[jax.ShapeDtypeStruct(w.shape, BF) for w in ws],
        compiler_params=pltpu.CompilerParams(vmem_limit_bytes=24 * MIB),
        cost_estimate=pl.CostEstimate(flops=8_000_000, bytes_accessed=12_000_000, transcendentals=0),
        name="arrange",
    )(place, *ws)


def by_expert(pieces, e):
    width = pieces[0].shape[1] // 2
    return jnp.concatenate([p[:, e * width : (e + 1) * width] for p in pieces], axis=1)


def grads_kernel(split, *refs):
    down_ref, dz_ref = refs[-2:]
    gs = piece_values(split, refs[:-2])
    for e in range(2):
        dz_ref[e] = dot(by_expert(gs, e), down_ref[e], NT)


def expert_grads(gs, down):
    flat, specs = piece_specs(gs, 128)
    rows, hidden = gs[0].shape[0], down.shape[1]
    return pl.pallas_call(
        lambda *refs: grads_kernel([isinstance(g, tuple) for g in gs], *refs),
        grid=(4,),
        in_specs=specs + [whole(down)],
        out_specs=pl.BlockSpec((2, 128, hidden), lambda r: (0, r, 0)),
        out_shape=jax.ShapeDtypeStruct((2, rows, hidden), F32),
        compiler_params=pltpu.CompilerParams(vmem_limit_bytes=24 * MIB),
        cost_estimate=pl.CostEstimate(flops=1_000_000_000, bytes_accessed=8_000_000, transcendentals=0),
        name="expert_grads",
    )(*flat, down)


def store_parts(vs, width, refs):
    def part(k):
        cut = slice(k * width, (k + 1) * width)
        return jnp.concatenate([v[:, cut] for v in vs], axis=1).astype(BF)

    own_ref, b_ref, a_ref, z_ref, minus_ref, plus_ref, cross_ref, near_ref = refs
    first_half = pl.program_id(0) < 2
    own_ref[...], b_ref[...], a_ref[...], z_ref[...] = part(0), part(1), part(3), part(4)
    c, zb, zc, za = part(2), part(5), part(6), part(7)

    @pl.when(first_half)
    def _():
        minus_ref[0] = zc
        minus_ref[1] = c
        cross_ref[...] = zb
        near_ref[...] = za

    @pl.when(jnp.logical_not(first_half))
    def _():
        plus_ref[0] = zc
        plus_ref[1] = c
        cross_ref[...] = za
        near_ref[...] = zb


def part_outputs(rows, width):
    block = pl.BlockSpec((128, width), lambda r: (r, 0))
    low = pl.BlockSpec((2, 128, width), lambda r: (0, jnp.minimum(r, 1), 0))
    high = pl.BlockSpec((2, 128, width), lambda r: (0, jnp.maximum(r - 2, 0), 0))
    one = jax.ShapeDtypeStruct((rows, width), BF)
    two = jax.ShapeDtypeStruct((2, rows // 2, width), BF)
    return [block] * 4 + [low, high, block, block], [one] * 4 + [two, two, one, one]


def rows_kernel(split, n_in, *refs):
    gate_ref, up_ref, dz_ref, z_ref = refs[n_in : n_in + 4]
    x_refs = refs[n_in + 4 :]
    us = piece_values(split, refs[:n_in])
    xs = []
    for e in range(2):
        u = by_expert(us, e)
        a = dot(u, gate_ref[e], NT)
        b = dot(u, up_ref[e], NT)
        dz = dz_ref[e]
        sig = jax.nn.sigmoid(a)
        silu = a * sig
        z_ref[e] = (silu * b).astype(BF)
        da = (dz * b * sig * (1.0 + a * (1.0 - sig))).astype(BF)
        db = (dz * silu).astype(BF)
        xs.append(dot(da, gate_ref[e], NN) + dot(db, up_ref[e], NN))
    store_parts(xs, us[0].shape[1] // 2, x_refs)


def expert_rows(us, gate, up, dz):
    flat, specs = piece_specs(us, 128)
    rows, width = us[0].shape
    hidden = gate.shape[1]
    part = pl.BlockSpec((2, 128, hidden), lambda r: (0, r, 0))
    out_specs, out_shape = part_outputs(rows, width)
    out = pl.pallas_call(
        lambda *refs: rows_kernel([isinstance(u, tuple) for u in us], len(flat), *refs),
        grid=(4,),
        in_specs=specs + [whole(gate), whole(up), part],
        out_specs=[part] + out_specs,
        out_shape=[jax.ShapeDtypeStruct((2, rows, hidden), BF)] + out_shape,
        compiler_params=pltpu.CompilerParams(vmem_limit_bytes=32 * MIB),
        cost_estimate=pl.CostEstimate(flops=4_000_000_000, bytes_accessed=15_000_000, transcendentals=200_000),
        name="expert_rows",
    )(*flat, gate, up, dz)
    return out[0], list(out[1:])


def outs_kernel(z_ref, down_ref, *y_refs):
    ys = [dot(z_ref[e], down_ref[e], NN) for e in range(2)]
    store_parts(ys, y_refs[0].shape[1] // 2, y_refs)


def expert_outs(z, down):
    out_specs, out_shape = part_outputs(z.shape[1], 2 * down.shape[2] // (NX * NZ))
    return list(
        pl.pallas_call(
            outs_kernel,
            grid=(4,),
            in_specs=[pl.BlockSpec((2, 128, z.shape[2]), lambda r: (0, r, 0)), whole(down)],
            out_specs=out_specs,
            out_shape=out_shape,
            compiler_params=pltpu.CompilerParams(vmem_limit_bytes=24 * MIB),
            cost_estimate=pl.CostEstimate(flops=1_000_000_000, bytes_accessed=8_000_000, transcendentals=0),
            name="expert_outs",
        )(z, down)
    )


def block_terms(d, feats_ref, turned_ref, pre, hidden):
    vis, out_part = feats_ref.shape[0] // 32, turned_ref.shape[0] // 32
    term_in = dot(feats_ref[pl.ds(pl.multiple_of(d * vis, 16), vis), :], pre, NT)
    term_out = dot(turned_ref[pl.ds(pl.multiple_of(d * out_part, 16), out_part), :], hidden, NT)
    both = jnp.concatenate([term_in, term_out], axis=0)
    h = both.shape[0] // 2
    return jnp.concatenate([both[:h], both[h:]], axis=1)


def sent_kernel(place_ref, turned_ref, w_ref, slope_ref, hidden_ref, feats_ref, pre_ref, out_ref):
    z = pl.program_id(0)
    dz, dy, dc = place_ref[0], place_ref[1], place_ref[2]

    @pl.when(z == 0)
    def _():
        pre_ref[...] = (dot(w_ref[...], turned_ref[...], NN) * slope_ref[...]).astype(BF)

    for y in range(RY):
        d = (lax.rem(dz + z, RZ) * RY + lax.rem(dy + y, RY)) * 2 + (1 - dc)
        terms = block_terms(d, feats_ref, turned_ref, pre_ref[...], hidden_ref[...])
        out_ref[y, 0] = terms.astype(BF)


def kept_kernel(place_ref, pre_ref, turned_ref, hidden_ref, feats_ref, got_ref, *out_refs):
    z = pl.program_id(0)
    dz, dy, dc = place_ref[0], place_ref[1], place_ref[2]
    sums = []
    for y in range(RY):
        d = (lax.rem(dz + z, RZ) * RY + lax.rem(dy + y, RY)) * 2 + dc
        terms = block_terms(d, feats_ref, turned_ref, pre_ref[...], hidden_ref[...])
        sums.append(terms + got_ref[y, 0].astype(F32))
    own, high, far, low = sums
    h = own.shape[0] // 2
    own_ref, minus_ref, plus_ref, near_ref = out_refs
    own_ref[0] = own.astype(BF)
    minus_ref[0] = joined(far[:h], low[h:]).astype(BF)
    plus_ref[0] = joined(far[h:], high[:h]).astype(BF)
    near_ref[0] = joined(low[:h], high[h:]).astype(BF)


def sent_terms(place, turned, proj_out, slope, hidden, feats):
    hid, rows = hidden.shape
    share = (feats.shape[0] + proj_out.shape[1]) // 32

    def full(w):
        return pl.BlockSpec(w.shape, lambda r, p: (0,) * w.ndim)

    pre = jax.ShapeDtypeStruct((hid, rows), BF)
    shape = (RY, RZ, share // 2, 2 * hid)
    return pl.pallas_call(
        sent_kernel,
        grid_spec=pltpu.PrefetchScalarGridSpec(
            num_scalar_prefetch=1,
            grid=(RZ,),
            in_specs=[full(turned), full(proj_out), full(slope), full(hidden), full(feats)],
            out_specs=[full(pre), pl.BlockSpec((RY, 1) + shape[2:], lambda r, p: (0, r, 0, 0))],
        ),
        out_shape=[pre, jax.ShapeDtypeStruct(shape, BF)],
        compiler_params=pltpu.CompilerParams(vmem_limit_bytes=24 * MIB),
        cost_estimate=pl.CostEstimate(flops=600_000_000, bytes_accessed=7_000_000, transcendentals=0),
        name="sent_terms",
    )(place, turned, proj_out, slope, hidden, feats)


def kept_terms(place, pre, turned, hidden, feats, got):
    def full(w):
        return pl.BlockSpec(w.shape, lambda r, p: (0,) * w.ndim)

    share, hid = got.shape[2:]
    return pl.pallas_call(
        kept_kernel,
        grid_spec=pltpu.PrefetchScalarGridSpec(
            num_scalar_prefetch=1,
            grid=(RZ,),
            in_specs=[full(pre), full(turned), full(hidden), full(feats)]
            + [pl.BlockSpec((RY, 1, share, hid), lambda r, p: (0, r, 0, 0))],
            out_specs=[pl.BlockSpec((1, share, hid), lambda r, p: (r, 0, 0))] * RY,
        ),
        out_shape=[jax.ShapeDtypeStruct((RZ, share, hid), BF)] * RY,
        compiler_params=pltpu.CompilerParams(vmem_limit_bytes=24 * MIB),
        cost_estimate=pl.CostEstimate(flops=400_000_000, bytes_accessed=7_000_000, transcendentals=0),
        name="kept_terms",
    )(place, pre, turned, hidden, feats, got)


def tied(first, *others):
    return lax.optimization_barrier((first, *others))[0]


def gelu_parts(preact):
    def smooth(values):
        return jax.nn.gelu(values, approximate=True)

    result, pullback = jax.vjp(smooth, preact)
    return (result, pullback(jnp.ones_like(preact))[0])


def adamw_update(weight, gradient, first, second):
    first_new = BETA_ONE * first + (1.0 - BETA_ONE) * gradient
    second_new = BETA_TWO * second + (1.0 - BETA_TWO) * gradient * gradient
    update = first_new / FIRST_FIX / (jnp.sqrt(second_new / SECOND_FIX) + EPSILON)
    current = weight.astype(F32)
    return (
        (current - LEARN_RATE * (update + WEIGHT_DECAY * current)).astype(BF),
        first_new,
        second_new,
    )


def rolled(v, axis, by):
    n = v.shape[axis]
    return lax.dynamic_slice_in_dim(jnp.concatenate([v, v], axis), by, n, axis)


def routing(routes, gate_weights):
    rows = routes.shape[0]
    names = jnp.arange(EXPERTS, dtype=jnp.int32)[:, None]
    hit = jnp.zeros((EXPERTS, rows), F32)
    weight = jnp.zeros((EXPERTS, rows), F32)
    for k in range(TOP):
        same = routes[:, k][None, :] == names
        hit = hit + same.astype(F32)
        weight = weight + jnp.where(same, gate_weights[:, k][None, :], 0.0)
    t = jnp.arange(rows, dtype=jnp.int32)
    before = (t[:, None] < t[None, :]).astype(BF)
    count = jnp.dot(hit.astype(BF), before, preferred_element_type=F32)
    place = jnp.where(hit > 0.0, count, -1.0)
    slots = jnp.arange(SLOTS, dtype=F32)[None, :, None]
    chosen, weighted = [], []
    for e in range(2):
        sel = place.reshape(EXPERTS // 2, 2, rows)[:, e][:, None, :] == slots
        w = weight.reshape(EXPERTS // 2, 2, rows)[:, e][:, None, :]
        chosen.append(sel.astype(BF).reshape(-1, rows))
        weighted.append(jnp.where(sel, w, 0.0).reshape(-1, rows))
    return chosen, weighted


def over_slots(v, sel, precision=None):
    return lax.dot_general(
        v, sel, (((0,), (0,)), ((), ())), precision=precision, preferred_element_type=F32
    )


def local(
    features,
    proj_in,
    proj_out,
    expert_gate,
    expert_up,
    expert_down,
    routes,
    gate_weights,
    cotangent,
    first_in,
    second_in,
    first_out,
    second_out,
):
    rows, model_width = cotangent.shape
    i = lax.axis_index("dp")
    j = lax.axis_index("mp")
    dz, dy, dc = i // (RY * 2), i // 2 % RY, i % 2
    mz, mx = j // NX, j % NX
    width = model_width // (NX * NZ)
    vis = features.shape[1] // 32

    turned_feats = features.T
    feats = turned_feats.reshape(RZ, RY, 2, vis, rows)
    feats = rolled(rolled(rolled(feats, 0, dz), 1, dy), 2, dc)
    feats = jnp.concatenate([feats[:, :2], feats[:, 3:], feats[:, 2:3]], 1)
    feats = jnp.transpose(feats, (2, 1, 0, 3, 4)).reshape(2, -1, rows)

    z_own, z_high, far_a, far_b, z_low = gather_ring(proj_in, lambda v, k: dp_send(v, dz=k))
    column = jnp.concatenate([z_own, z_high, far_a, far_b, z_low], 0)
    y_own, y_high, y_far_a, y_far_b, y_low = gather_ring(column, lambda v, k: dp_send(v, dy=k))
    plane = (jnp.concatenate([y_own, y_high, y_low], 0), jnp.concatenate([y_far_a, y_far_b], 0))
    chosen, weighted = routing(routes, gate_weights)
    cot_cols = lax.dynamic_slice_in_dim(cotangent, j * width, width, 1)

    def picked_grads(e):
        w = jnp.sum(weighted[e], axis=1, keepdims=True)
        return (w * jnp.dot(chosen[e], cot_cols, preferred_element_type=F32)).astype(BF)

    send_grads = jnp.concatenate([picked_grads(0), picked_grads(1)], 1)
    own_grads = a2a_dp(tied(send_grads, z_low, z_high))
    *plane, own_grads = lax.optimization_barrier((*plane, own_grads))
    near_grads = gather_near(own_grads)
    other = [dp_send(p, dc=1) for p in plane]
    cut = plane[0].shape[0]

    preact = (
        over_slots(plane[0], feats[0, :cut])
        + over_slots(plane[1], feats[0, cut:])
        + over_slots(other[0], feats[1, :cut])
        + over_slots(other[1], feats[1, cut:])
    )
    activated, gelu_slope = gelu_parts(preact)
    hidden = activated.astype(BF)
    partial_value = lax.dot_general(
        proj_out, hidden, (((0,), (0,)), ((), ())), preferred_element_type=F32
    ).astype(BF)
    partial_value, *near_grads = lax.optimization_barrier((partial_value, *near_grads))
    arrived = lax.all_to_all(
        partial_value.reshape(NX * NZ, width, rows), "mp", split_axis=0, concat_axis=0, tiled=True
    )
    gate, up, down = arranged(
        jnp.stack([mz, mx]).astype(jnp.int32),
        jnp.swapaxes(expert_gate, 1, 2),
        jnp.swapaxes(expert_up, 1, 2),
        expert_down,
    )
    arrived, gate, up, down = lax.optimization_barrier((arrived, gate, up, down))
    mapped_cols = jnp.sum(arrived.astype(F32), axis=0).astype(BF)

    send_rows = jnp.concatenate([dot(chosen[e], mapped_cols, NT).astype(BF) for e in range(2)], 1)
    grad_parts = gather_far(own_grads, *near_grads)
    own_rows = a2a_dp(send_rows)
    own_rows, *grad_parts = lax.optimization_barrier((own_rows, *grad_parts))
    near_rows = gather_near(own_rows)
    inner_grads = expert_grads(piece_order(*grad_parts), down)
    inner_grads, *near_rows = lax.optimization_barrier((inner_grads, *near_rows))
    row_parts = piece_order(*gather_far(own_rows, *near_rows))

    inner, x_parts = expert_rows(row_parts, gate, up, inner_grads)
    y_parts = expert_outs(inner, down)
    x_sum = scatter_near(x_parts, scatter_far(x_parts))
    back_in = a2a_dp(x_sum)
    back_in, *y_parts = lax.optimization_barrier((back_in, *y_parts))
    y_far = scatter_far(y_parts)
    grad_cols = (
        cot_cols.T.astype(F32)
        + over_slots(back_in[:, :width], chosen[0])
        + over_slots(back_in[:, width:], chosen[1])
    ).astype(BF)

    def by_columns(cols):
        same = jnp.broadcast_to(cols[None], (NX * NZ,) + cols.shape)
        got = lax.all_to_all(same, "mp", split_axis=0, concat_axis=0, tiled=True)
        return got.reshape(model_width, rows)

    place = jnp.stack([dz, dy, dc]).astype(jnp.int32)
    turned, *y_far = lax.optimization_barrier((by_columns(grad_cols), *y_far))
    y_sum = scatter_near(y_parts, y_far)
    pre, sent = sent_terms(place, turned, proj_out, gelu_slope, hidden, turned_feats)
    got = dp_send(sent, dc=1)
    kept, minus, plus, near = kept_terms(place, pre, turned, hidden, turned_feats, got)
    early = (dp_send(minus, dy=-1), dp_send(plus, dy=1))
    *early, y_sum = lax.optimization_barrier((*early, y_sum))
    back_out = a2a_dp(y_sum)
    total = scatter_end(kept, near, early, lambda v, k: dp_send(v, dy=k)).astype(BF)
    total, back_out = lax.optimization_barrier((total, back_out))
    shares = scatter_ring(*(total[k] for k in range(RZ)), lambda v, k: dp_send(v, dz=k))
    shares = jnp.concatenate([shares[:, : shares.shape[1] // 2], shares[:, shares.shape[1] // 2 :]], 0)
    grad_in = shares[:vis]
    grad_out = shares[vis:].T

    moe_cols = (
        mapped_cols.astype(F32)
        + over_slots(back_out[:, :width].astype(F32), weighted[0], lax.Precision.HIGHEST)
        + over_slots(back_out[:, width:].astype(F32), weighted[1], lax.Precision.HIGHEST)
    ).astype(BF)
    moe_out = by_columns(moe_cols).T

    out_part = model_width // 32
    own_out = lax.dynamic_slice_in_dim(proj_out, i * out_part, out_part, 1)
    new_in, first_in_new, second_in_new = adamw_update(proj_in, grad_in, first_in, second_in)
    new_out, first_out_new, second_out_new = adamw_update(own_out, grad_out, first_out, second_out)
    return (moe_out, new_in, new_out, first_in_new, second_in_new, first_out_new, second_out_new)


def solution(mesh):
    return jax.shard_map(
        local,
        mesh=mesh,
        in_specs=(
            P("dp", None),
            P("dp", "mp"),
            P("mp", None),
            P("dp", None, "mp"),
            P("dp", None, "mp"),
            P("dp", "mp", None),
            P("dp", None),
            P("dp", None),
            P("dp", None),
            P("dp", "mp"),
            P("dp", "mp"),
            P("mp", "dp"),
            P("mp", "dp"),
        ),
        out_specs=(
            P("dp", None),
            P("dp", "mp"),
            P("mp", "dp"),
            P("dp", "mp"),
            P("dp", "mp"),
            P("mp", "dp"),
            P("mp", "dp"),
        ),
        check_vma=False,
    )
```

```python
import jax
import jax.numpy as jnp
from jax import lax
from jax.experimental import pallas as pl
from jax.experimental.pallas import tpu as pltpu
from jax.sharding import PartitionSpec as P

EXPERTS = 64
TOP = 6
SLOTS = 16
NX, NZ = 4, 2
RY, RZ = 4, 4

BETA_ONE = 0.9
BETA_TWO = 0.999
EPSILON = 1e-08
LEARN_RATE = 0.001
WEIGHT_DECAY = 0.1
FIRST_FIX = 1.0 - 0.9**50 * 0.9**50
SECOND_FIX = 1.0 - 0.999**50 * 0.999**50

BF = jnp.bfloat16
F32 = jnp.float32


def mp_send(v, dx, dz=0):
    pairs = [
        (z * NX + x, (z + dz) % NZ * NX + (x + dx) % NX) for z in range(NZ) for x in range(NX)
    ]
    return lax.ppermute(v, "mp", pairs)


def dp_send(v, dz=0, dy=0, dc=0):
    pairs = [
        ((z * RY + y) * 2 + c, ((z + dz) % RZ * RY + (y + dy) % RY) * 2 + (c + dc) % 2)
        for z in range(RZ)
        for y in range(RY)
        for c in range(2)
    ]
    return lax.ppermute(v, "dp", pairs)


def add(*terms):
    total = terms[0].astype(F32)
    for t in terms[1:]:
        total = total + t.astype(F32)
    return total.astype(BF)


def gather_ring(v, send):
    h = v.shape[0] // 2
    low = send(v, 1)
    high = send(v, -1)
    far_a = send(low[:h], 1)
    far_b = send(high[h:], -1)
    return v, high, far_a, far_b, low


def scatter_start(own, high, far, low, send):
    h = own.shape[-2] // 2
    early = (
        send(far[..., :h, :], -1),
        send(far[..., h:, :], 1),
        send(low[..., h:, :], -1),
        send(high[..., :h, :], 1),
    )
    return early, (own, low[..., :h, :], high[..., h:, :])


def scatter_end(early, late, send):
    own, low_a, high_b = late
    r_a, r_b, s_b, s_a = early
    h = own.shape[-2] // 2
    t_a = send(add(low_a, r_a), -1)
    t_b = send(add(high_b, r_b), 1)
    return jnp.concatenate(
        [
            own[..., :h, :].astype(F32) + s_a.astype(F32) + t_a.astype(F32),
            own[..., h:, :].astype(F32) + s_b.astype(F32) + t_b.astype(F32),
        ],
        -2,
    )


def scatter_ring(own, high, far, low, send):
    return scatter_end(*scatter_start(own, high, far, low, send), send)


def gather_near(u):
    return mp_send(u, 1), mp_send(u, -1), mp_send(u, 0, 1)


def gather_far(u, a, b, z):
    h = u.shape[0] // 2
    c_lo = mp_send(a[:h], 1)
    c_hi = mp_send(b[h:], -1)
    za_lo = mp_send(z[:h], 1)
    zb_hi = mp_send(z[h:], -1)
    za_hi = mp_send(a[h:], 0, 1)
    zb_lo = mp_send(b[:h], 0, 1)
    zc_lo = mp_send(za_lo, 1)
    zc_hi = mp_send(zb_hi, -1)
    return [u, b, (c_lo, c_hi), a, z, (zb_lo, zb_hi), (zc_lo, zc_hi), (za_lo, za_hi)]


def scatter_far(parts):
    own, b, c, a, z, zb, zc, za = parts
    h = own.shape[0] // 2
    return (
        mp_send(zc[:h], -1),
        mp_send(zc[h:], 1),
        mp_send(c[:h], -1),
        mp_send(c[h:], 1),
        mp_send(za[h:], 0, 1),
        mp_send(zb[:h], 0, 1),
    )


def scatter_near(parts, far):
    own, b, c, a, z, zb, zc, za = parts
    r1, r2, r3, r5, r7, r8 = far
    h = own.shape[0] // 2
    r4 = mp_send(add(za[:h], r1), -1)
    r6 = mp_send(add(zb[h:], r2), 1)
    r9 = mp_send(add(a, jnp.concatenate([r3, r7], 0)), -1)
    r10 = mp_send(add(b, jnp.concatenate([r8, r5], 0)), 1)
    r11 = mp_send(add(z, jnp.concatenate([r4, r6], 0)), 0, 1)
    return add(own, r9, r10, r11)


def a2a_dp(v):
    w = v.reshape(32, SLOTS, v.shape[-1])
    return lax.all_to_all(w, "dp", split_axis=0, concat_axis=0, tiled=True).reshape(v.shape)


NT = (((1,), (1,)), ((), ()))
NN = (((1,), (0,)), ((), ()))
MIB = 1024 * 1024


def dot(x, y, dims):
    return lax.dot_general(x, y, dims, preferred_element_type=F32)


def piece_specs(pieces, block):
    flat, specs = [], []
    for p in pieces:
        if isinstance(p, tuple):
            flat += list(p)
            width = p[0].shape[1]
            specs.append(pl.BlockSpec((block, width), lambda r: (jnp.minimum(r, 1), 0)))
            specs.append(pl.BlockSpec((block, width), lambda r: (jnp.maximum(r - 2, 0), 0)))
        else:
            flat.append(p)
            specs.append(pl.BlockSpec((block, p.shape[1]), lambda r: (r, 0)))
    return flat, specs


def piece_values(split, refs):
    first_half = pl.program_id(0) < 2
    out, at = [], 0
    for s in split:
        if s:
            out.append(jnp.where(first_half, refs[at][...], refs[at + 1][...]))
            at += 2
        else:
            out.append(refs[at][...])
            at += 1
    return out


def whole(w):
    return pl.BlockSpec(w.shape, lambda r: (0,) * w.ndim)


def arrange_kernel(place_ref, *refs):
    mz, mx = place_ref[0], place_ref[1]
    for src, dst in zip(refs[:3], refs[3:]):
        half = src.shape[2] // NZ
        step = half // NX
        for k in range(NZ):
            at = pl.multiple_of(lax.rem(mz + k, NZ) * half, half)
            v = src[0, :, pl.ds(at, half)]
            for x in range(NX):

                @pl.when(mx == x)
                def _(v=v, x=x, k=k, dst=dst):
                    turned = v if x == 0 else jnp.concatenate([v[:, x * step :], v[:, : x * step]], 1)
                    dst[0, :, k * half : (k + 1) * half] = turned


def arranged(place, *ws):
    spec = pl.BlockSpec((1,) + ws[0].shape[1:], lambda e, p: (e, 0, 0))
    return pl.pallas_call(
        arrange_kernel,
        grid_spec=pltpu.PrefetchScalarGridSpec(
            num_scalar_prefetch=1, grid=(2,), in_specs=[spec] * 3, out_specs=[spec] * 3
        ),
        out_shape=[jax.ShapeDtypeStruct(w.shape, BF) for w in ws],
        compiler_params=pltpu.CompilerParams(vmem_limit_bytes=24 * MIB),
        cost_estimate=pl.CostEstimate(flops=8_000_000, bytes_accessed=12_000_000, transcendentals=0),
        name="arrange",
    )(place, *ws)


def by_expert(pieces, e):
    width = pieces[0].shape[1] // 2
    return jnp.concatenate([p[:, e * width : (e + 1) * width] for p in pieces], axis=1)


def grads_kernel(split, *refs):
    down_ref, dz_ref = refs[-2:]
    gs = piece_values(split, refs[:-2])
    for e in range(2):
        dz_ref[e] = dot(by_expert(gs, e), down_ref[e], NT)


def expert_grads(gs, down):
    flat, specs = piece_specs(gs, 128)
    rows, hidden = gs[0].shape[0], down.shape[1]
    return pl.pallas_call(
        lambda *refs: grads_kernel([isinstance(g, tuple) for g in gs], *refs),
        grid=(4,),
        in_specs=specs + [whole(down)],
        out_specs=pl.BlockSpec((2, 128, hidden), lambda r: (0, r, 0)),
        out_shape=jax.ShapeDtypeStruct((2, rows, hidden), F32),
        compiler_params=pltpu.CompilerParams(vmem_limit_bytes=24 * MIB),
        cost_estimate=pl.CostEstimate(flops=1_000_000_000, bytes_accessed=8_000_000, transcendentals=0),
        name="expert_grads",
    )(*flat, down)


def rows_kernel(split, n_in, *refs):
    gate_ref, up_ref, dz_ref, z_ref = refs[n_in : n_in + 4]
    x_refs = refs[n_in + 4 :]
    us = piece_values(split, refs[:n_in])
    xs = []
    for e in range(2):
        u = by_expert(us, e)
        a = dot(u, gate_ref[e], NT)
        b = dot(u, up_ref[e], NT)
        dz = dz_ref[e]
        sig = jax.nn.sigmoid(a)
        silu = a * sig
        z_ref[e] = (silu * b).astype(BF)
        da = (dz * b * sig * (1.0 + a * (1.0 - sig))).astype(BF)
        db = (dz * silu).astype(BF)
        xs.append(dot(da, gate_ref[e], NN) + dot(db, up_ref[e], NN))
    width = us[0].shape[1] // 2
    for k, ref in enumerate(x_refs):
        cut = slice(k * width, (k + 1) * width)
        ref[...] = jnp.concatenate([x[:, cut] for x in xs], axis=1).astype(BF)


def expert_rows(us, gate, up, dz):
    flat, specs = piece_specs(us, 128)
    rows, width = us[0].shape
    hidden = gate.shape[1]
    part = pl.BlockSpec((2, 128, hidden), lambda r: (0, r, 0))
    out = pl.pallas_call(
        lambda *refs: rows_kernel([isinstance(u, tuple) for u in us], len(flat), *refs),
        grid=(4,),
        in_specs=specs + [whole(gate), whole(up), part],
        out_specs=[part] + [pl.BlockSpec((128, width), lambda r: (r, 0))] * len(us),
        out_shape=[jax.ShapeDtypeStruct((2, rows, hidden), BF)]
        + [jax.ShapeDtypeStruct((rows, width), BF)] * len(us),
        compiler_params=pltpu.CompilerParams(vmem_limit_bytes=32 * MIB),
        cost_estimate=pl.CostEstimate(flops=4_000_000_000, bytes_accessed=15_000_000, transcendentals=200_000),
        name="expert_rows",
    )(*flat, gate, up, dz)
    return out[0], list(out[1:])


def outs_kernel(z_ref, down_ref, *y_refs):
    ys = [dot(z_ref[e], down_ref[e], NN) for e in range(2)]
    width = y_refs[0].shape[1] // 2
    for k, ref in enumerate(y_refs):
        cut = slice(k * width, (k + 1) * width)
        ref[...] = jnp.concatenate([y[:, cut] for y in ys], axis=1).astype(BF)


def expert_outs(z, down, count):
    rows = z.shape[1]
    width = 2 * down.shape[2] // count
    return list(
        pl.pallas_call(
            outs_kernel,
            grid=(4,),
            in_specs=[pl.BlockSpec((2, 128, z.shape[2]), lambda r: (0, r, 0)), whole(down)],
            out_specs=[pl.BlockSpec((128, width), lambda r: (r, 0))] * count,
            out_shape=[jax.ShapeDtypeStruct((rows, width), BF)] * count,
            compiler_params=pltpu.CompilerParams(vmem_limit_bytes=24 * MIB),
            cost_estimate=pl.CostEstimate(flops=1_000_000_000, bytes_accessed=8_000_000, transcendentals=0),
            name="expert_outs",
        )(z, down)
    )


def block_terms(d, feats_ref, turned_ref, pre, hidden):
    vis, out_part = feats_ref.shape[0] // 32, turned_ref.shape[0] // 32
    term_in = dot(feats_ref[pl.ds(pl.multiple_of(d * vis, 16), vis), :], pre, NT)
    term_out = dot(turned_ref[pl.ds(pl.multiple_of(d * out_part, 16), out_part), :], hidden, NT)
    both = jnp.concatenate([term_in, term_out], axis=0)
    h = both.shape[0] // 2
    return jnp.concatenate([both[:h], both[h:]], axis=1).astype(BF)


def sent_kernel(place_ref, turned_ref, w_ref, slope_ref, hidden_ref, feats_ref, pre_ref, out_ref):
    z = pl.program_id(0)
    dz, dy, dc = place_ref[0], place_ref[1], place_ref[2]

    @pl.when(z == 0)
    def _():
        pre_ref[...] = (dot(w_ref[...], turned_ref[...], NN) * slope_ref[...]).astype(BF)

    for y in range(RY):
        d = (lax.rem(dz + z, RZ) * RY + lax.rem(dy + y, RY)) * 2 + (1 - dc)
        out_ref[y, 0] = block_terms(d, feats_ref, turned_ref, pre_ref[...], hidden_ref[...])


def kept_kernel(place_ref, pre_ref, turned_ref, hidden_ref, feats_ref, got_ref, *out_refs):
    z = pl.program_id(0)
    dz, dy, dc = place_ref[0], place_ref[1], place_ref[2]
    for y in range(RY):
        d = (lax.rem(dz + z, RZ) * RY + lax.rem(dy + y, RY)) * 2 + dc
        terms = block_terms(d, feats_ref, turned_ref, pre_ref[...], hidden_ref[...])
        out_refs[y][0] = (terms.astype(F32) + got_ref[y, 0].astype(F32)).astype(BF)


def sent_terms(place, turned, proj_out, slope, hidden, feats):
    hid, rows = hidden.shape
    share = (feats.shape[0] + proj_out.shape[1]) // 32

    def full(w):
        return pl.BlockSpec(w.shape, lambda r, p: (0,) * w.ndim)

    pre = jax.ShapeDtypeStruct((hid, rows), BF)
    shape = (RY, RZ, share // 2, 2 * hid)
    return pl.pallas_call(
        sent_kernel,
        grid_spec=pltpu.PrefetchScalarGridSpec(
            num_scalar_prefetch=1,
            grid=(RZ,),
            in_specs=[full(turned), full(proj_out), full(slope), full(hidden), full(feats)],
            out_specs=[full(pre), pl.BlockSpec((RY, 1) + shape[2:], lambda r, p: (0, r, 0, 0))],
        ),
        out_shape=[pre, jax.ShapeDtypeStruct(shape, BF)],
        compiler_params=pltpu.CompilerParams(vmem_limit_bytes=24 * MIB),
        cost_estimate=pl.CostEstimate(flops=600_000_000, bytes_accessed=7_000_000, transcendentals=0),
        name="sent_terms",
    )(place, turned, proj_out, slope, hidden, feats)


def kept_terms(place, pre, turned, hidden, feats, got):
    def full(w):
        return pl.BlockSpec(w.shape, lambda r, p: (0,) * w.ndim)

    share, hid = got.shape[2:]
    return pl.pallas_call(
        kept_kernel,
        grid_spec=pltpu.PrefetchScalarGridSpec(
            num_scalar_prefetch=1,
            grid=(RZ,),
            in_specs=[full(pre), full(turned), full(hidden), full(feats)]
            + [pl.BlockSpec((RY, 1, share, hid), lambda r, p: (0, r, 0, 0))],
            out_specs=[pl.BlockSpec((1, share, hid), lambda r, p: (r, 0, 0))] * RY,
        ),
        out_shape=[jax.ShapeDtypeStruct((RZ, share, hid), BF)] * RY,
        compiler_params=pltpu.CompilerParams(vmem_limit_bytes=24 * MIB),
        cost_estimate=pl.CostEstimate(flops=400_000_000, bytes_accessed=7_000_000, transcendentals=0),
        name="kept_terms",
    )(place, pre, turned, hidden, feats, got)


def tied(first, *others):
    return lax.optimization_barrier((first, *others))[0]


def gelu_parts(preact):
    def smooth(values):
        return jax.nn.gelu(values, approximate=True)

    result, pullback = jax.vjp(smooth, preact)
    return (result, pullback(jnp.ones_like(preact))[0])


def adamw_update(weight, gradient, first, second):
    first_new = BETA_ONE * first + (1.0 - BETA_ONE) * gradient
    second_new = BETA_TWO * second + (1.0 - BETA_TWO) * gradient * gradient
    update = first_new / FIRST_FIX / (jnp.sqrt(second_new / SECOND_FIX) + EPSILON)
    current = weight.astype(F32)
    return (
        (current - LEARN_RATE * (update + WEIGHT_DECAY * current)).astype(BF),
        first_new,
        second_new,
    )


def rolled(v, axis, by):
    n = v.shape[axis]
    return lax.dynamic_slice_in_dim(jnp.concatenate([v, v], axis), by, n, axis)


def routing(routes, gate_weights):
    rows = routes.shape[0]
    names = jnp.arange(EXPERTS, dtype=jnp.int32)[:, None]
    hit = jnp.zeros((EXPERTS, rows), F32)
    weight = jnp.zeros((EXPERTS, rows), F32)
    for k in range(TOP):
        same = routes[:, k][None, :] == names
        hit = hit + same.astype(F32)
        weight = weight + jnp.where(same, gate_weights[:, k][None, :], 0.0)
    t = jnp.arange(rows, dtype=jnp.int32)
    before = (t[:, None] < t[None, :]).astype(BF)
    count = jnp.dot(hit.astype(BF), before, preferred_element_type=F32)
    place = jnp.where(hit > 0.0, count, -1.0)
    slots = jnp.arange(SLOTS, dtype=F32)[None, :, None]
    chosen, weighted = [], []
    for e in range(2):
        sel = place.reshape(EXPERTS // 2, 2, rows)[:, e][:, None, :] == slots
        w = weight.reshape(EXPERTS // 2, 2, rows)[:, e][:, None, :]
        chosen.append(sel.astype(BF).reshape(-1, rows))
        weighted.append(jnp.where(sel, w, 0.0).reshape(-1, rows))
    return chosen, weighted


def over_slots(v, sel, precision=None):
    return lax.dot_general(
        v, sel, (((0,), (0,)), ((), ())), precision=precision, preferred_element_type=F32
    )


def local(
    features,
    proj_in,
    proj_out,
    expert_gate,
    expert_up,
    expert_down,
    routes,
    gate_weights,
    cotangent,
    first_in,
    second_in,
    first_out,
    second_out,
):
    rows, model_width = cotangent.shape
    i = lax.axis_index("dp")
    j = lax.axis_index("mp")
    dz, dy, dc = i // (RY * 2), i // 2 % RY, i % 2
    mz, mx = j // NX, j % NX
    width = model_width // (NX * NZ)
    vis = features.shape[1] // 32

    turned_feats = features.T
    feats = turned_feats.reshape(RZ, RY, 2, vis, rows)
    feats = rolled(rolled(rolled(feats, 0, dz), 1, dy), 2, dc)
    feats = jnp.transpose(feats, (2, 1, 0, 3, 4)).reshape(-1, rows)

    own, high, far_a, far_b, low = gather_ring(proj_in, lambda v, k: dp_send(v, dz=k))
    column = jnp.concatenate([own, high, far_a, far_b, low], 0)
    plane = gather_ring(column, lambda v, k: dp_send(v, dy=k))
    other = [dp_send(p, dc=1) for p in plane]
    weights_in = jnp.concatenate(list(plane) + other, 0)

    chosen, weighted = routing(routes, gate_weights)
    cot_cols = lax.dynamic_slice_in_dim(cotangent, j * width, width, 1)

    def picked_grads(e):
        w = jnp.sum(weighted[e], axis=1, keepdims=True)
        return (w * jnp.dot(chosen[e], cot_cols, preferred_element_type=F32)).astype(BF)

    send_grads = jnp.concatenate([picked_grads(0), picked_grads(1)], 1)
    own_grads = a2a_dp(tied(send_grads, plane[1], plane[4]))

    preact = lax.dot_general(
        weights_in, feats, (((0,), (0,)), ((), ())), preferred_element_type=F32
    )
    activated, gelu_slope = gelu_parts(preact)
    hidden = activated.astype(BF)
    partial_value = lax.dot_general(
        proj_out, hidden, (((0,), (0,)), ((), ())), preferred_element_type=F32
    ).astype(BF)
    partial_value, own_grads = lax.optimization_barrier((partial_value, own_grads))
    near_grads = gather_near(own_grads)
    arrived = lax.all_to_all(
        partial_value.reshape(NX * NZ, width, rows), "mp", split_axis=0, concat_axis=0, tiled=True
    )
    mapped_cols = jnp.sum(arrived.astype(F32), axis=0).astype(BF)

    send_rows = jnp.concatenate([dot(chosen[e], mapped_cols, NT).astype(BF) for e in range(2)], 1)
    grad_parts = gather_far(own_grads, *near_grads)
    own_rows = a2a_dp(send_rows)
    leaves, tree = jax.tree.flatten(grad_parts)
    own_rows, *leaves = lax.optimization_barrier((own_rows, *leaves))
    grad_parts = jax.tree.unflatten(tree, leaves)
    row_parts = gather_far(own_rows, *gather_near(own_rows))
    gate, up, down = arranged(
        jnp.stack([mz, mx]).astype(jnp.int32),
        jnp.swapaxes(expert_gate, 1, 2),
        jnp.swapaxes(expert_up, 1, 2),
        expert_down,
    )
    inner_grads = expert_grads(grad_parts, down)

    inner, x_parts = expert_rows(row_parts, gate, up, inner_grads)
    y_parts = expert_outs(inner, down, len(x_parts))
    x_sum = scatter_near(x_parts, scatter_far(x_parts))
    back_in = a2a_dp(x_sum)
    grad_cols = (
        cot_cols.T.astype(F32)
        + over_slots(back_in[:, :width], chosen[0])
        + over_slots(back_in[:, width:], chosen[1])
    ).astype(BF)

    def by_columns(cols):
        same = jnp.broadcast_to(cols[None], (NX * NZ,) + cols.shape)
        got = lax.all_to_all(same, "mp", split_axis=0, concat_axis=0, tiled=True)
        return got.reshape(model_width, rows)

    place = jnp.stack([dz, dy, dc]).astype(jnp.int32)
    turned = by_columns(grad_cols)
    *y_parts, turned = lax.optimization_barrier((*y_parts, turned))
    y_far = scatter_far(y_parts)
    pre, sent = sent_terms(place, turned, proj_out, gelu_slope, hidden, turned_feats)
    got = dp_send(sent, dc=1)
    total = kept_terms(place, pre, turned, hidden, turned_feats, got)
    early, late = scatter_start(*total, lambda v, k: dp_send(v, dy=k))
    out = lax.optimization_barrier((*early, *y_far))
    early, y_far = out[: len(early)], out[len(early) :]
    back_out = a2a_dp(scatter_near(y_parts, y_far))
    total = scatter_end(early, late, lambda v, k: dp_send(v, dy=k)).astype(BF)
    shares = scatter_ring(*(total[k] for k in range(RZ)), lambda v, k: dp_send(v, dz=k))
    shares, back_out = lax.optimization_barrier((shares, back_out))
    shares = jnp.concatenate([shares[:, : shares.shape[1] // 2], shares[:, shares.shape[1] // 2 :]], 0)
    grad_in = shares[:vis]
    grad_out = shares[vis:].T

    moe_cols = (
        mapped_cols.astype(F32)
        + over_slots(back_out[:, :width].astype(F32), weighted[0], lax.Precision.HIGHEST)
        + over_slots(back_out[:, width:].astype(F32), weighted[1], lax.Precision.HIGHEST)
    ).astype(BF)
    moe_out = by_columns(moe_cols).T

    out_part = model_width // 32
    own_out = lax.dynamic_slice_in_dim(proj_out, i * out_part, out_part, 1)
    new_in, first_in_new, second_in_new = adamw_update(proj_in, grad_in, first_in, second_in)
    new_out, first_out_new, second_out_new = adamw_update(own_out, grad_out, first_out, second_out)
    return (moe_out, new_in, new_out, first_in_new, second_in_new, first_out_new, second_out_new)


def solution(mesh):
    return jax.shard_map(
        local,
        mesh=mesh,
        in_specs=(
            P("dp", None),
            P("dp", "mp"),
            P("mp", None),
            P("dp", None, "mp"),
            P("dp", None, "mp"),
            P("dp", "mp", None),
            P("dp", None),
            P("dp", None),
            P("dp", None),
            P("dp", "mp"),
            P("dp", "mp"),
            P("mp", "dp"),
            P("mp", "dp"),
        ),
        out_specs=(
            P("dp", None),
            P("dp", "mp"),
            P("mp", "dp"),
            P("dp", "mp"),
            P("dp", "mp"),
            P("mp", "dp"),
            P("mp", "dp"),
        ),
        check_vma=False,
    )
```
